32 devices in a mesh: gx: 4 (over y, core), gy: 4 (over z), gz: 2 (over x).
Axes of the slice: x: 2, y: 2, z: 4, core: 2. Of those that a mesh axis runs over, the one named last changes fastest.
Arguments:
- moments: float32 [8, 16, 64, 1024], P(None, 'gx', 'gy', 'gz'), may hold values from 0.001 to 60, as said below
- velocity: float32 [3, 16, 64, 1024], P(None, 'gx', 'gy', 'gz'), may hold values from -4 to 4
- drift: float32 [3, 16, 64, 1024], P(None, 'gx', 'gy', 'gz'), may hold values from -8 to 8
Outputs:
- updated: float32 [8, 16, 64, 1024], P(None, 'gx', 'gy', 'gz')
- totals: float32 [8], replicated
The draws below stay inside these ranges and needn't reach their ends.
Inputs may be any that keep to these rules, and one draw needn't show every extreme that they name: In every cell the 8 entries are the moments of order 0 to 7 of a log-normal distribution of particle size.
All inputs are finite; a program needn't handle non-finite values. Where the reference program divides by a largest or mean magnitude, that divisor is 1e-20 or more.
Results may differ from the reference program's by a relative error of at most 0.0003.
Values sent between devices are 32-bit elements; how exact they have to be, the bound alone decides.
A program may use at most 64 MiB of HBM per device.

```python
import jax
import jax.numpy as jnp
from jax import lax

SWEEPS = 6
NX = 16
NY = 64
NZ = 1024


def draw_moments(key, part):
    keys = jax.random.split(key, 3)
    shape = (NX, NY, NZ)
    place_x = lax.broadcasted_iota(jnp.float32, shape, 0) / NX
    place_y = lax.broadcasted_iota(jnp.float32, shape, 1) / NY
    place_z = lax.broadcasted_iota(jnp.float32, shape, 2) / NZ
    ramp = 1.0 + 2.0 * (place_x + place_y + place_z) / 3.0
    rough = jnp.exp(jax.random.uniform(keys[0], shape, jnp.float32, -0.35, 0.35))
    width = jax.random.uniform(keys[1], shape, jnp.float32, 0.3, 0.8)
    offset = jax.random.uniform(keys[2], shape, jnp.float32, -0.2, 0.2)
    number = ramp * rough
    variance = width * width
    center = -3.5 * variance + offset
    orders = jnp.arange(8, dtype=jnp.float32)[:, None, None, None]
    return number[None] * jnp.exp(orders * center[None] + 0.5 * orders * orders * variance[None])


def shard_levels(own_key, shape, pieces, smallest, top_value):
    level, own = 1.0, jax.random.fold_in(own_key, 6)
    for position, shards_of in pieces:
        heights = jnp.exp(jax.random.uniform(jax.random.fold_in(own, position), (shards_of,), jnp.float32, smallest / len(pieces), top_value / len(pieces)))
        level = level * jnp.repeat(heights, shape[position] // shards_of).reshape([-1 if axis == position else 1 for axis in range(len(shape))])
    return level


def scatter_about(own_key, dims, scale, reach, cuts=(), kind=jnp.bfloat16):
    array = scale * jax.random.normal(own_key, dims, jnp.float32)
    if cuts:
        array = array * shard_levels(own_key, dims, cuts, -0.22, 0.18)
    return jnp.clip(array, -reach, reach).astype(kind)


def setup_inputs(seed: int = 0) -> dict:
    splits = jax.random.split(jax.random.key(seed), 4)
    return {
        "moments": draw_moments(jax.random.fold_in(splits[3], 71), 0),
        "velocity": scatter_about(splits[1], (3, NX, NY, NZ), 1.0, 4.0, ((1, 4), (2, 4), (3, 2)), jnp.float32),
        "drift": scatter_about(splits[2], (3, NX, NY, NZ), 2.0, 8.0, ((1, 4), (2, 4), (3, 2)), jnp.float32),
    }


cfl_number = 0.4
speed_eps = 1e-06
pair_list = ((0, 1), (0, 2), (0, 3), (1, 2), (1, 3), (2, 3))

def entry_key(first_index, second_index):
    return (min(first_index, second_index), max(first_index, second_index))

def invert(moment):
    levels = [moment[order] for order in range(8)]
    zeros = jnp.zeros_like(levels[0])
    before = [zeros] * 8
    alphas = [levels[1] / levels[0]]
    betas = [levels[0]]
    for level in range(1, 4):
        fresh = [zeros] * 8
        for column in range(level, 8 - level):
            fresh[column] = levels[column + 1] - alphas[level - 1] * levels[column] - betas[level - 1] * before[column]
        alphas.append(fresh[level + 1] / fresh[level] - levels[level] / levels[level - 1])
        betas.append(fresh[level] / levels[level - 1])
        before, levels = (levels, fresh)
    table = {}
    for row_index in range(4):
        for col_index in range(row_index, 4):
            table[row_index, col_index] = zeros
    for row_index in range(4):
        table[row_index, row_index] = alphas[row_index]
    for row_index in range(3):
        table[row_index, row_index + 1] = jnp.sqrt(betas[row_index + 1])
    first = [jnp.ones_like(zeros), zeros, zeros, zeros]
    for _ in range(SWEEPS):
        for pivot, other in pair_list:
            coupling = table[pivot, other]
            head = table[pivot, pivot]
            tail = table[other, other]
            spread = tail - head
            orient = jnp.where(spread >= 0, 1.0, -1.0)
            tangent = orient * 2.0 * coupling / (jnp.abs(spread) + jnp.sqrt(spread * spread + 4.0 * coupling * coupling))
            cosine = 1.0 / jnp.sqrt(1.0 + tangent * tangent)
            sine = tangent * cosine
            for rest in range(4):
                if rest != pivot and rest != other:
                    near = table[entry_key(rest, pivot)]
                    far = table[entry_key(rest, other)]
                    table[entry_key(rest, pivot)] = cosine * near - sine * far
                    table[entry_key(rest, other)] = sine * near + cosine * far
            table[pivot, pivot] = head - tangent * coupling
            table[other, other] = tail + tangent * coupling
            table[pivot, other] = jnp.zeros_like(coupling)
            first_p = first[pivot]
            first_q = first[other]
            first[pivot] = cosine * first_p - sine * first_q
            first[other] = sine * first_p + cosine * first_q
    weights = [moment[0] * first[node] * first[node] for node in range(4)]
    places = [table[node, node] for node in range(4)]
    return jnp.stack(weights + places)

def face_flux(extended, axis, count):

    def part(channel, start):
        return lax.slice_in_dim(extended[channel], start, start + count + 1, axis=axis - 1)
    mean_speed = 0.5 * (part(8, 0) + part(8, 1))
    mean_drift = 0.5 * (part(9, 0) + part(9, 1))
    zeros = jnp.zeros_like(mean_speed)
    accum = [zeros] * 8
    for node in range(4):
        for start, upwind in ((0, jnp.maximum), (1, jnp.minimum)):
            size = part(4 + node, start)
            carried = part(node, start) * upwind(mean_speed + mean_drift * size, 0.0)
            for order in range(8):
                accum[order] = accum[order] + carried
                carried = carried * size
    return jnp.stack(accum)

def reference(moments, velocity, drift):
    nodes = jnp.moveaxis(lax.map(invert, jnp.moveaxis(moments, 1, 0)), 0, 1)
    change = jnp.zeros_like(moments)
    for direction in range(3):
        axis = direction + 1
        count = moments.shape[axis]
        pack = jnp.concatenate([nodes, velocity[direction:direction + 1], drift[direction:direction + 1]], 0)
        widths = [(0, 0), (0, 0), (0, 0), (0, 0)]
        widths[axis] = (1, 1)
        if direction < 2:
            extended = jnp.pad(pack, widths, mode='wrap')
        else:
            extended = jnp.pad(pack, widths)
        flux = face_flux(extended, axis, count)
        if direction == 2:
            face = lax.broadcasted_iota(jnp.int32, flux.shape, 3)
            flux = jnp.where((face == 0) | (face == count), 0.0, flux)
        change = change + lax.slice_in_dim(flux, 1, count + 1, axis=axis) - lax.slice_in_dim(flux, 0, count, axis=axis)
    speed = jnp.zeros_like(moments[0])
    for direction in range(3):
        speed = speed + lax.optimization_barrier(jnp.max(jnp.abs(velocity[direction][None] + drift[direction][None] * nodes[4:8]), axis=0))
    step_size = cfl_number / (jnp.max(speed) + speed_eps)
    updated = moments - step_size * change
    totals = lax.optimization_barrier(jnp.sum(updated, axis=(1, 2, 3))) / (NX * NY * NZ)
    return (updated, totals)
```

```python
import functools

import jax
import jax.numpy as jnp
from jax import lax
from jax.experimental import pallas as pl
from jax.experimental.pallas import tpu as pltpu
from jax.sharding import PartitionSpec as P

SWEEPS = 6
AXES = ("gx", "gy", "gz")
LANES = 128
SUBLANES = 8

cfl_number = 0.4
speed_eps = 1e-06
pair_list = ((0, 1), (0, 2), (0, 3), (1, 2), (1, 3), (2, 3))


def entry_key(i, j):
    return (min(i, j), max(i, j))


def scaled(scale, value):
    return value if scale is None else scale * value


def sheared(alpha, beta, near, far):
    if near is None and far is None:
        return None, None
    if near is None:
        return -(alpha * far), far
    if far is None:
        return near, beta * near
    return near - alpha * far, far + beta * near


def recurrence(moment):
    levels = list(moment)
    before = None
    inverse = 1.0 / levels[0]
    ratios = [levels[1] * inverse]
    alphas = [ratios[0]]
    betas = [levels[0]]
    for level in range(1, 4):
        fresh = [None] * 8
        for column in range(level, 8 - level):
            value = levels[column + 1] - alphas[level - 1] * levels[column]
            if level > 1:
                value = value - betas[level - 1] * before[column]
            fresh[column] = value
        betas.append(fresh[level] * inverse)
        inverse = 1.0 / fresh[level]
        ratios.append(fresh[level + 1] * inverse)
        alphas.append(ratios[level] - ratios[level - 1])
        before, levels = levels, fresh
    return alphas, betas


def invert(moment):
    diag, betas = recurrence(moment)
    table = {(i, j): None for i in range(4) for j in range(i + 1, 4)}
    for i in range(3):
        table[i, i + 1] = 2.0 * jnp.sqrt(betas[i + 1])
    scale = [None] * 4
    first = [1.0, None, None, None]
    for _ in range(SWEEPS):
        for p, q in pair_list:
            entry = table[p, q]
            if entry is None:
                continue
            spread = diag[q] - diag[p]
            left = scaled(scale[p], entry)
            right = scaled(scale[q], entry)
            r = lax.rsqrt(spread * spread + left * right)
            r = jnp.where(spread >= 0, r, -r)
            wide = 1.0 + spread * r
            turn = r / wide
            alpha = right * turn
            beta = left * turn
            shift = 0.5 * (left * alpha)
            half = 0.5 * wide
            scale[p] = scaled(scale[p], half)
            scale[q] = scaled(scale[q], half)
            for rest in range(4):
                if rest not in (p, q):
                    a, b = entry_key(rest, p), entry_key(rest, q)
                    table[a], table[b] = sheared(alpha, beta, table[a], table[b])
            diag[p] = diag[p] - shift
            diag[q] = diag[q] + shift
            table[p, q] = None
            first[p], first[q] = sheared(alpha, beta, first[p], first[q])
    weights = [moment[0] * (scale[i] * (first[i] * first[i])) for i in range(4)]
    return weights, diag


def outflow(weights, sizes, mean_speed, mean_drift, upwind):
    sums = None
    for w, s in zip(weights, sizes):
        term = w * upwind(mean_speed + mean_drift * s, 0.0)
        terms = [term]
        for _ in range(7):
            term = term * s
            terms.append(term)
        sums = terms if sums is None else [a + b for a, b in zip(sums, terms)]
    return sums


def kernel(
    sizes, m_hbm, v_hbm, g_hbm, out, tot_ref,
    m, v, g, nodes, acc, fx, zp, zm, yu, zu,
    hvx, vy_s, vy_r, vz_s, vz_r, y_s, y_r, z_s, z_r, table,
    in_sem, nb_send, nb_recv, all_sem, plane_sem,
):
    X, Y, Z = m.shape[1:]
    count = sizes[0] * sizes[1] * sizes[2]
    zc = Z // LANES
    at = [lax.axis_index(a) for a in AXES]
    me = (at[0] * sizes[1] + at[1]) * sizes[2] + at[2]
    row = lax.broadcasted_iota(jnp.int32, (Y, LANES), 0)
    lane = lax.broadcasted_iota(jnp.int32, (Y, LANES), 1)
    bottom = at[2] == 0
    top = at[2] == sizes[2] - 1

    def along(axis, step):
        return lax.rem(at[axis] + step + sizes[axis], sizes[axis])

    def beside(axis, step):
        place = list(at)
        place[axis] = along(axis, step)
        return tuple(place)

    edge = [0] if X == 1 else [0, X - 1]
    inner = list(range(1, X - 1))
    loads = [pltpu.make_async_copy(m_hbm.at[:, x], m.at[:, x], in_sem.at[x]) for x in range(X)]
    loads_v = pltpu.make_async_copy(v_hbm, v, in_sem.at[X])
    loads_g = pltpu.make_async_copy(g_hbm, g, in_sem.at[X + 1])
    for x in edge:
        loads[x].start()
    loads_v.start()
    loads_g.start()
    for x in inner:
        loads[x].start()

    barrier = pltpu.get_barrier_semaphore()
    xs = [along(0, i) for i in range(sizes[0])]
    zs_ = [along(2, i) for i in range(sizes[2])]
    plane = [
        (xs[i], at[1], zs_[j]) for i in range(sizes[0]) for j in range(sizes[2]) if i or j
    ]
    line = [(at[0], along(1, i), at[2]) for i in range(1, sizes[1])]
    for place in plane + line:
        pl.semaphore_signal(
            barrier, inc=1, device_id=place, device_id_type=pl.DeviceIdType.MESH
        )

    sent = []

    def send(src, dst, axis, step):
        index = len(sent)
        copy = pltpu.make_async_remote_copy(
            src_ref=src, dst_ref=dst, send_sem=nb_send.at[index], recv_sem=nb_recv.at[index],
            device_id=beside(axis, step), device_id_type=pl.DeviceIdType.MESH,
        )
        copy.start()
        sent.append(copy)
        return copy

    def solve(layers):
        weights, places = invert(
            [jnp.concatenate([m[k, x] for x in layers], axis=0) for k in range(8)]
        )
        for n, x in enumerate(layers):
            for i in range(4):
                nodes[x + 1, i] = weights[i][n * Y : (n + 1) * Y]
                nodes[x + 1, 4 + i] = places[i][n * Y : (n + 1) * Y]

    def fastest(x):
        speed = None
        for d in range(3):
            vd, gd = v[d, x], g[d, x]
            parts = [jnp.abs(vd + gd * nodes[x + 1, 4 + i]) for i in range(4)]
            largest = jnp.maximum(
                jnp.maximum(parts[0], parts[1]), jnp.maximum(parts[2], parts[3])
            )
            speed = largest if speed is None else speed + largest
        return speed

    for x in edge:
        loads[x].wait()
    solve(edge)
    loads_v.wait()
    loads_g.wait()
    for x in range(X):
        for part, ref in ((0, v), (1, g)):
            vy_s[0, x, part : part + 1, :] = ref[1, x, Y - 1 : Y, :]
            vy_s[1, x, part : part + 1, :] = ref[1, x, 0:1, :]
        high = [ref[2, x, :, Z - LANES : Z] for ref in (v, g)]
        low = [ref[2, x, :, 0:LANES] for ref in (v, g)]
        vz_s[0, x] = jnp.where(lane == 0, pltpu.roll(high[0], 1, 1), pltpu.roll(high[1], 2, 1))
        vz_s[1, x] = jnp.where(lane == 0, low[0], pltpu.roll(low[1], 1, 1))
    pl.semaphore_wait(barrier, len(plane) + len(line))
    velocity_copies = [
        send(vy_s.at[0], vy_r.at[0], 1, 1),
        send(vy_s.at[1], vy_r.at[1], 1, -1),
        send(vz_s.at[0], vz_r.at[0], 2, 1),
        send(vz_s.at[1], vz_r.at[1], 2, -1),
        send(v.at[0, X - 1], hvx.at[0, 0], 0, 1),
        send(g.at[0, X - 1], hvx.at[0, 1], 0, 1),
        send(v.at[0, 0], hvx.at[1, 0], 0, -1),
        send(g.at[0, 0], hvx.at[1, 1], 0, -1),
    ]
    x_copies = [
        send(nodes.at[1], nodes.at[X + 1], 0, -1),
        send(nodes.at[X], nodes.at[0], 0, 1),
    ]
    for place in line:
        pl.semaphore_signal(
            plane_sem, inc=1, device_id=place, device_id_type=pl.DeviceIdType.MESH
        )

    for x in inner:
        loads[x].wait()
    if inner:
        solve(inner)
    best = functools.reduce(jnp.maximum, [fastest(x) for x in range(X)])

    def fold(value):
        value = functools.reduce(
            jnp.add, [value[i : i + SUBLANES, :] for i in range(0, value.shape[0], SUBLANES)]
        )
        return functools.reduce(
            jnp.add, [value[:, i : i + LANES] for i in range(0, value.shape[1], LANES)]
        )

    def lanes_of(chunk):
        return pl.ds(pl.multiple_of(chunk * LANES, LANES), LANES)

    def nodes_of(layer, zs, ys=slice(None)):
        return (
            [nodes[layer, i, ys, zs] for i in range(4)],
            [nodes[layer, 4 + i, ys, zs] for i in range(4)],
        )

    for copy in velocity_copies[:4]:
        copy.wait_recv()

    def means(x, carry):
        for part, ref in ((0, v), (1, g)):
            here = ref[1, x]
            wide_row = lax.broadcasted_iota(jnp.int32, (Y, Z), 0)
            after = vy_r[1, x, part : part + 1, :]
            ahead = vy_r[0, x, part : part + 1, :]
            yu[x, part] = 0.5 * (
                here + jnp.where(wide_row == Y - 1, after, pltpu.roll(here, Y - 1, 0))
            )
            yu[x, 2 + part] = 0.5 * (
                here + jnp.where(wide_row == 0, ahead, pltpu.roll(here, 1, 0))
            )
            here = ref[2, x]
            after = pltpu.roll(vz_r[1, x], LANES - 1 - part, 1)
            ahead = pltpu.roll(vz_r[0, x], LANES - part, 1) if part else vz_r[0, x]
            up = pltpu.roll(here, Z - 1, 1)
            down = pltpu.roll(here, 1, 1)
            for c in range(zc):
                zs = slice(c * LANES, (c + 1) * LANES)
                u, d = up[:, zs], down[:, zs]
                if c == zc - 1:
                    u = jnp.where(lane == LANES - 1, after, u)
                if c == 0:
                    d = jnp.where(lane == 0, ahead, d)
                zu[x, part, :, zs] = 0.5 * (here[:, zs] + u)
                zu[x, 2 + part, :, zs] = 0.5 * (here[:, zs] + d)
        return carry

    lax.fori_loop(0, X, means, 0)

    def side_y(x, carry):
        last = slice(Y - SUBLANES, Y)
        high = outflow(*nodes_of(x + 1, slice(None), last), yu[x, 0, last], yu[x, 1, last], jnp.maximum)
        begin = slice(0, SUBLANES)
        low = outflow(*nodes_of(x + 1, slice(None), begin), yu[x, 2, begin], yu[x, 3, begin], jnp.minimum)
        for k in range(8):
            y_s[0, x, k : k + 1, :] = high[k][SUBLANES - 1 : SUBLANES, :]
            y_s[1, x, k : k + 1, :] = low[k][0:1, :]
        return carry

    lax.fori_loop(0, X, side_y, 0)
    y_copies = [send(y_s.at[0], y_r.at[0], 1, 1), send(y_s.at[1], y_r.at[1], 1, -1)]

    def side_z(x, carry):
        zs = slice(Z - LANES, Z)
        high = outflow(*nodes_of(x + 1, zs), zu[x, 0, :, zs], zu[x, 1, :, zs], jnp.maximum)
        zs = slice(0, LANES)
        low = outflow(*nodes_of(x + 1, zs), zu[x, 2, :, zs], zu[x, 3, :, zs], jnp.minimum)
        packed_high = jnp.zeros((Y, LANES), jnp.float32)
        packed_low = jnp.zeros((Y, LANES), jnp.float32)
        for k in range(8):
            packed_high = jnp.where(lane == k, pltpu.roll(high[k], k + 1, 1), packed_high)
            packed_low = jnp.where(
                lane == k, pltpu.roll(low[k], k, 1) if k else low[k], packed_low
            )
        z_s[0, x] = jnp.where(top, 0.0, packed_high)
        z_s[1, x] = jnp.where(bottom, 0.0, packed_low)
        return carry

    lax.fori_loop(0, X, side_z, 0)
    z_copies = [send(z_s.at[0], z_r.at[0], 2, 1), send(z_s.at[1], z_r.at[1], 2, -1)]

    for copy in velocity_copies[4:]:
        copy.wait_recv()

    def drift_of(x, zs):
        return v[0, x, :, zs], g[0, x, :, zs]

    def between(left, right):
        return 0.5 * (left[0] + right[0]), 0.5 * (left[1] + right[1])

    def side_x(i, sums):
        zs = lanes_of(i)
        ahead = between((hvx[0, 0, :, zs], hvx[0, 1, :, zs]), drift_of(0, zs))
        after = between(drift_of(X - 1, zs), (hvx[1, 0, :, zs], hvx[1, 1, :, zs]))
        upper = outflow(*nodes_of(X, zs), *after, jnp.maximum)
        lower = outflow(*nodes_of(1, zs), *ahead, jnp.minimum)
        return tuple(a + fold(b) for a, b in zip(sums, upper + lower))

    zero = jnp.zeros((SUBLANES, LANES), jnp.float32)
    x_sums = lax.fori_loop(0, zc, side_x, (zero,) * 16)

    def mass(x, sums):
        return tuple(s + fold(m[k, x]) for k, s in enumerate(sums))

    m_sums = lax.fori_loop(0, X, mass, (zero,) * 8)

    tile_row = lax.broadcasted_iota(jnp.int32, (SUBLANES, LANES), 0)
    tile_lane = lax.broadcasted_iota(jnp.int32, (SUBLANES, LANES), 1)

    def stacked(sums):
        block = zero
        for k in range(8):
            block = jnp.where(tile_row == k, jnp.sum(sums[k], axis=0, keepdims=True), block)
        return block

    blocks = [stacked(m_sums), stacked(x_sums[:8]), stacked(x_sums[8:])]
    for side in range(2):
        part = functools.reduce(jnp.add, [y_s[side, x] for x in range(X)])
        blocks.append(
            functools.reduce(jnp.add, [part[:, i : i + LANES] for i in range(0, Z, LANES)])
        )
    packed = zero
    for n, block in enumerate(blocks):
        value = jnp.sum(block, axis=1, keepdims=True)
        packed = jnp.where(tile_lane == tile_row + 8 * (n + 1), value, packed)
    for side in range(2):
        part = functools.reduce(jnp.add, [z_s[side, x] for x in range(X)])
        part = functools.reduce(
            jnp.add, [part[i : i + SUBLANES] for i in range(0, Y, SUBLANES)]
        )
        packed = packed + pltpu.roll(
            jnp.where(tile_lane < 8, part, 0.0), 8 * (len(blocks) + 1 + side), 1
        )
    packed = jnp.sum(packed, axis=0, keepdims=True)
    best = functools.reduce(
        jnp.maximum,
        [best[i : i + SUBLANES, j : j + LANES]
         for i in range(0, Y, SUBLANES) for j in range(0, Z, LANES)],
    )
    best = jnp.max(jnp.max(best, axis=0, keepdims=True), axis=1, keepdims=True)
    one_lane = lax.broadcasted_iota(jnp.int32, (1, LANES), 1)
    table[me] = jnp.where(one_lane == 0, best, packed)

    pl.semaphore_wait(plane_sem, len(line))

    def spread(j, carry):
        place = jnp.where(j >= me, j + 1, j)
        pltpu.make_async_remote_copy(
            src_ref=table.at[me], dst_ref=table.at[me],
            send_sem=all_sem.at[0], recv_sem=all_sem.at[1],
            device_id=place, device_id_type=pl.DeviceIdType.LOGICAL,
        ).start()
        return carry

    lax.fori_loop(0, count - 1, spread, 0)

    def side_faces(i, carry):
        x, chunk = lax.div(i, zc), lax.rem(i, zc)
        zs = lanes_of(chunk)
        w, s = nodes_of(x + 1, zs)
        high = outflow(w, s, yu[x, 0, :, zs], yu[x, 1, :, zs], jnp.maximum)
        for k in range(8):
            acc[x, k, :, zs] = high[k] - jnp.where(row == 0, 0.0, pltpu.roll(high[k], 1, 0))
        low = outflow(w, s, yu[x, 2, :, zs], yu[x, 3, :, zs], jnp.minimum)
        for k in range(8):
            acc[x, k, :, zs] += (
                jnp.where(row == Y - 1, 0.0, pltpu.roll(low[k], Y - 1, 0)) - low[k]
            )
        return carry

    lax.fori_loop(0, X * zc, side_faces, 0)

    def wall_faces(i, carry):
        x, chunk = lax.div(i, zc), lax.rem(i, zc)
        zs = lanes_of(chunk)
        w, s = nodes_of(x + 1, zs)
        shut_high = (lane == LANES - 1) & ((chunk == zc - 1) & top)
        shut_low = (lane == 0) & ((chunk == 0) & bottom)
        high = outflow(w, s, zu[x, 0, :, zs], zu[x, 1, :, zs], jnp.maximum)
        for k in range(8):
            zp[x, k, :, zs] = jnp.where(shut_high, 0.0, high[k])
        low = outflow(w, s, zu[x, 2, :, zs], zu[x, 3, :, zs], jnp.minimum)
        for k in range(8):
            zm[x, k, :, zs] = jnp.where(shut_low, 0.0, low[k])
        return carry

    lax.fori_loop(0, X * zc, wall_faces, 0)

    def face_x(face, zs, left, right):
        mean = between(left, right)
        upper = outflow(*nodes_of(face, zs), *mean, jnp.maximum)
        lower = outflow(*nodes_of(face + 1, zs), *mean, jnp.minimum)
        for k in range(8):
            fx[face, k, :, zs] = upper[k] + lower[k]

    def inner_x(i, carry):
        face, zs = lax.div(i, zc) + 1, lanes_of(lax.rem(i, zc))
        face_x(face, zs, drift_of(face - 1, zs), drift_of(face, zs))
        return carry

    def outer_x(i, carry):
        zs = lanes_of(i)
        face_x(0, zs, (hvx[0, 0, :, zs], hvx[0, 1, :, zs]), drift_of(0, zs))
        face_x(X, zs, drift_of(X - 1, zs), (hvx[1, 0, :, zs], hvx[1, 1, :, zs]))
        return carry

    if X > 1:
        lax.fori_loop(0, (X - 1) * zc, inner_x, 0)

    for copy in x_copies:
        copy.wait_recv()
    lax.fori_loop(0, zc, outer_x, 0)
    for copy in y_copies + z_copies:
        copy.wait_recv()

    wide_row = lax.broadcasted_iota(jnp.int32, (Y, Z), 0)
    wide_lane = lax.broadcasted_iota(jnp.int32, (Y, Z), 1)

    def combine(x, carry):
        low_all, high_all = z_r[0, x], z_r[1, x]
        for k in range(8):
            fp, fm = zp[x, k], zm[x, k]
            first = pltpu.roll(low_all, LANES - k, 1) if k else low_all
            last = pltpu.roll(high_all, LANES - 1 - k, 1)
            spare = [first] * (zc - 1)
            before = jnp.where(
                wide_lane == 0, jnp.concatenate([first] + spare, 1), pltpu.roll(fp, 1, 1)
            )
            spare = [last] * (zc - 1)
            after = jnp.where(
                wide_lane == Z - 1, jnp.concatenate(spare + [last], 1), pltpu.roll(fm, Z - 1, 1)
            )
            change = acc[x, k] + ((fp + after) - (fm + before))
            change = change + (fx[x + 1, k] - fx[x, k])
            change = change + jnp.where(
                wide_row == Y - 1, y_r[1, x, k : k + 1, :],
                jnp.where(wide_row == 0, -y_r[0, x, k : k + 1, :], 0.0),
            )
            acc[x, k] = change
        return carry

    lax.fori_loop(0, X, combine, 0)

    every = pltpu.make_async_copy(
        table.at[pl.ds(0, count - 1)], table.at[pl.ds(0, count - 1)], all_sem.at[1]
    )
    every.wait()
    rows = table[...]
    largest = jnp.max(jnp.max(rows, axis=0)[:, 0:1], axis=1, keepdims=True)
    step = cfl_number / (largest + speed_eps)

    def update(x, carry):
        for k in range(8):
            out[k, x] = m[k, x] - step * acc[x, k]
        return carry

    lax.fori_loop(0, X, update, 0)

    grid = rows.reshape(sizes + (1, LANES))

    def turned(axis, step):
        size = sizes[axis]
        cut = (size - step) % size
        if cut == 0:
            return grid
        return jnp.concatenate(
            [lax.slice_in_dim(grid, cut, size, axis=axis), lax.slice_in_dim(grid, 0, cut, axis=axis)],
            axis=axis,
        )

    group = one_lane // 8
    net = jnp.zeros((1, LANES), jnp.float32)
    for axis in range(3):
        rise = jnp.sum((grid - turned(axis, 1)).reshape(count, 1, LANES), axis=0)
        fall = jnp.sum((turned(axis, -1) - grid).reshape(count, 1, LANES), axis=0)
        net = net + jnp.where(group == 2 + 2 * axis, rise, jnp.where(group == 3 + 2 * axis, fall, 0.0))
    net = jnp.broadcast_to(net, (SUBLANES, LANES))
    change = functools.reduce(jnp.add, [pltpu.roll(net, LANES - 8 * n, 1) for n in range(2, 8)])[0:1]
    both = pltpu.roll(jnp.broadcast_to(jnp.sum(rows, axis=0), (SUBLANES, LANES)), LANES - 8, 1)[0:1]
    tot_ref[...] = (both - step * change) / float(count * X * Y * Z)

    for copy in sent:
        copy.wait_send()
    pltpu.make_async_copy(
        table.at[pl.ds(0, count - 1)], table.at[pl.ds(0, count - 1)], all_sem.at[0]
    ).wait()


def shards(sizes, moments, velocity, drift):
    _, X, Y, Z = moments.shape
    count = sizes[0] * sizes[1] * sizes[2]
    f32 = jnp.float32
    vm = lambda *shape: pltpu.VMEM(shape, f32)
    updated, totals = pl.pallas_call(
        functools.partial(kernel, sizes),
        name="transport",
        out_shape=(
            pltpu.VMEM(moments.shape, f32), pltpu.VMEM((1, LANES), f32)
        ),
        in_specs=[pl.BlockSpec(memory_space=pl.ANY)] * 3,
        out_specs=(
            pl.BlockSpec(memory_space=pltpu.VMEM), pl.BlockSpec(memory_space=pltpu.VMEM)
        ),
        scratch_shapes=[
            vm(8, X, Y, Z), vm(3, X, Y, Z), vm(3, X, Y, Z), vm(X + 2, 8, Y, Z), vm(X, 8, Y, Z),
            vm(X + 1, 8, Y, Z), vm(X, 8, Y, Z), vm(X, 8, Y, Z), vm(X, 4, Y, Z), vm(X, 4, Y, Z),
            vm(2, 2, Y, Z), vm(2, X, 2, Z), vm(2, X, 2, Z), vm(2, X, Y, LANES),
            vm(2, X, Y, LANES), vm(2, X, 8, Z), vm(2, X, 8, Z), vm(2, X, Y, LANES),
            vm(2, X, Y, LANES), vm(count, 1, LANES),
            pltpu.SemaphoreType.DMA((X + 2,)),
            pltpu.SemaphoreType.DMA((14,)), pltpu.SemaphoreType.DMA((14,)),
            pltpu.SemaphoreType.DMA((2,)), pltpu.SemaphoreType.REGULAR,
        ],
        compiler_params=pltpu.CompilerParams(collective_id=0, has_side_effects=True),
    )(moments, velocity, drift)
    return updated, totals[0, :8]


def solution(mesh):
    spec = P(None, "gx", "gy", "gz")
    sizes = tuple(mesh.shape[a] for a in AXES)
    return jax.shard_map(
        functools.partial(shards, sizes), mesh=mesh, in_specs=(spec,) * 3,
        out_specs=(spec, P()), check_vma=False,
    )
```

```python
import functools

import jax
import jax.numpy as jnp
from jax import lax
from jax.experimental import pallas as pl
from jax.experimental.pallas import tpu as pltpu
from jax.sharding import PartitionSpec as P

SWEEPS = 6
EARLY_NODES = 5
EARLY_SWEEPS = 3
AXES = ("gx", "gy", "gz")
LANES = 128
SUBLANES = 8

cfl_number = 0.4
speed_eps = 1e-06
pair_list = ((0, 1), (0, 2), (0, 3), (1, 2), (1, 3), (2, 3))


def entry_key(i, j):
    return (min(i, j), max(i, j))


def scaled(scale, value):
    return value if scale is None else scale * value


def sheared(alpha, beta, near, far):
    if near is None and far is None:
        return None, None
    if near is None:
        return -(alpha * far), far
    if far is None:
        return near, beta * near
    return near - alpha * far, far + beta * near


def recurrence(moment):
    levels = list(moment)
    before = None
    inverse = 1.0 / levels[0]
    ratios = [levels[1] * inverse]
    alphas = [ratios[0]]
    betas = [levels[0]]
    for level in range(1, 4):
        fresh = [None] * 8
        for column in range(level, 8 - level):
            value = levels[column + 1] - alphas[level - 1] * levels[column]
            if level > 1:
                value = value - betas[level - 1] * before[column]
            fresh[column] = value
        betas.append(fresh[level] * inverse)
        inverse = 1.0 / fresh[level]
        ratios.append(fresh[level + 1] * inverse)
        alphas.append(ratios[level] - ratios[level - 1])
        before, levels = levels, fresh
    return alphas, betas


def begin(moment):
    diag, betas = recurrence(moment)
    table = {(i, j): None for i in range(4) for j in range(i + 1, 4)}
    for i in range(3):
        table[i, i + 1] = 2.0
    scale = [None, betas[1]]
    for i in range(2, 4):
        scale.append(betas[i] / scale[i - 1])
    return diag, table, scale, [1.0, None, None, None]


def sweep(state, sweeps):
    diag, table, scale, first = state
    for _ in range(sweeps):
        for p, q in pair_list:
            entry = table[p, q]
            if entry is None:
                continue
            spread = diag[q] - diag[p]
            left = scaled(scale[p], entry)
            right = scaled(scale[q], entry)
            r = lax.rsqrt(spread * spread + left * right)
            r = jnp.where(spread >= 0, r, -r)
            wide = 1.0 + spread * r
            turn = r / wide
            alpha = right * turn
            beta = left * turn
            shift = 0.5 * (left * alpha)
            half = 0.5 * wide
            scale[p] = scaled(scale[p], half)
            scale[q] = scaled(scale[q], half)
            for rest in range(4):
                if rest not in (p, q):
                    a, b = entry_key(rest, p), entry_key(rest, q)
                    table[a], table[b] = sheared(alpha, beta, table[a], table[b])
            diag[p] = diag[p] - shift
            diag[q] = diag[q] + shift
            table[p, q] = None
            first[p], first[q] = sheared(alpha, beta, first[p], first[q])


def quadrature(number, state):
    diag, table, scale, first = state
    return [number * (scale[i] * (first[i] * first[i])) for i in range(4)], diag


def outflow(weights, sizes, mean_speed, mean_drift, upwind):
    sums = None
    for w, s in zip(weights, sizes):
        term = w * upwind(mean_speed + mean_drift * s, 0.0)
        terms = [term]
        for _ in range(7):
            term = term * s
            terms.append(term)
        sums = terms if sums is None else [a + b for a, b in zip(sums, terms)]
    return sums


def kernel(
    sizes, m_hbm, v_hbm, g_hbm, out, tot_ref,
    m, v, g, nodes, acc, fx, zp, zm, yu, zu,
    hvx, vy_s, vy_r, vz_s, vz_r, y_s, y_r, z_s, z_r, y_face, z_face, table,
    in_sem, nb_send, nb_recv, all_sem, plane_sem,
):
    X, Y, Z = m.shape[1:]
    count = sizes[0] * sizes[1] * sizes[2]
    zc = Z // LANES
    at = [lax.axis_index(a) for a in AXES]
    me = (at[0] * sizes[1] + at[1]) * sizes[2] + at[2]
    row = lax.broadcasted_iota(jnp.int32, (Y, LANES), 0)
    lane = lax.broadcasted_iota(jnp.int32, (Y, LANES), 1)
    bottom = at[2] == 0
    top = at[2] == sizes[2] - 1

    def along(axis, step):
        return lax.rem(at[axis] + step + sizes[axis], sizes[axis])

    def beside(axis, step):
        place = list(at)
        place[axis] = along(axis, step)
        return tuple(place)

    edge = [0] if X == 1 else [0, X - 1]
    inner = list(range(1, X - 1))
    loads = [pltpu.make_async_copy(m_hbm.at[:, x], m.at[:, x], in_sem.at[x]) for x in range(X)]
    loads_v = pltpu.make_async_copy(v_hbm, v, in_sem.at[X])
    loads_g = pltpu.make_async_copy(g_hbm, g, in_sem.at[X + 1])
    for x in edge:
        loads[x].start()
    loads_v.start()
    loads_g.start()
    for x in inner:
        loads[x].start()

    barrier = pltpu.get_barrier_semaphore()
    xs = [along(0, i) for i in range(sizes[0])]
    zs_ = [along(2, i) for i in range(sizes[2])]
    plane = [
        (xs[i], at[1], zs_[j]) for i in range(sizes[0]) for j in range(sizes[2]) if i or j
    ]
    line = [(at[0], along(1, i), at[2]) for i in range(1, sizes[1])]
    for place in plane + line:
        pl.semaphore_signal(
            barrier, inc=1, device_id=place, device_id_type=pl.DeviceIdType.MESH
        )

    sent = []

    def send(src, dst, axis, step):
        index = len(sent)
        copy = pltpu.make_async_remote_copy(
            src_ref=src, dst_ref=dst, send_sem=nb_send.at[index], recv_sem=nb_recv.at[index],
            device_id=beside(axis, step), device_id_type=pl.DeviceIdType.MESH,
        )
        copy.start()
        sent.append(copy)
        return copy

    order = edge + inner
    columns = [jnp.zeros((Y, LANES), jnp.float32)] * 2

    def moments_of(layers, k):
        return jnp.concatenate([m[k, x] for x in layers], axis=0)

    def start(layers, sweeps):
        state = begin([moments_of(layers, k) for k in range(8)])
        sweep(state, sweeps)
        return state

    def solve(layers, state, sweeps):
        sweep(state, sweeps)
        weights, places = quadrature(moments_of(layers, 0), state)
        for n, x in enumerate(layers):
            for i in range(4):
                nodes[x + 1, i] = weights[i][n * Y : (n + 1) * Y]
                nodes[x + 1, 4 + i] = places[i][n * Y : (n + 1) * Y]
            for i, value in enumerate(weights + places):
                value = value[n * Y : (n + 1) * Y]
                p = order.index(x)
                for c in range(zc):
                    part = value[:, c * LANES : (c + 1) * LANES]
                    y_s[0, c, 8 * p + i : 8 * p + i + 1, :] = part[Y - 1 : Y]
                    y_s[1, c, 8 * p + i : 8 * p + i + 1, :] = part[0:1]
                spot = i * X + p
                for side, edge_lane in ((0, LANES - 1), (1, 0)):
                    tile = value[:, Z - LANES : Z] if side == 0 else value[:, 0:LANES]
                    turn = (spot - edge_lane) % LANES
                    tile = pltpu.roll(tile, turn, 1) if turn else tile
                    columns[side] = jnp.where(lane == spot, tile, columns[side])

    def fastest(x):
        speed = None
        for d in range(3):
            vd, gd = v[d, x], g[d, x]
            parts = [jnp.abs(vd + gd * nodes[x + 1, 4 + i]) for i in range(4)]
            largest = jnp.maximum(
                jnp.maximum(parts[0], parts[1]), jnp.maximum(parts[2], parts[3])
            )
            speed = largest if speed is None else speed + largest
        return speed

    for x in edge:
        loads[x].wait()
    state = start(edge, EARLY_SWEEPS)
    loads_v.wait()
    loads_g.wait()
    packs = [jnp.zeros((Y, LANES), jnp.float32)] * 2
    for p, x in enumerate(order):
        for part, ref in ((0, v), (1, g)):
            vy_s[0, part, p : p + 1, :] = ref[1, x, Y - 1 : Y, :]
            vy_s[1, part, p : p + 1, :] = ref[1, x, 0:1, :]
            spot = part * X + p
            tile = pltpu.roll(ref[2, x, :, Z - LANES : Z], spot + 1, 1)
            packs[0] = jnp.where(lane == spot, tile, packs[0])
            tile = ref[2, x, :, 0:LANES]
            tile = pltpu.roll(tile, spot, 1) if spot else tile
            packs[1] = jnp.where(lane == spot, tile, packs[1])
    for side in range(2):
        vz_s[side] = packs[side]
    pl.semaphore_wait(barrier, len(plane) + len(line))
    velocity_copies = [
        send(vy_s.at[0], vy_r.at[0], 1, 1),
        send(vy_s.at[1], vy_r.at[1], 1, -1),
        send(vz_s.at[0], vz_r.at[0], 2, 1),
        send(vz_s.at[1], vz_r.at[1], 2, -1),
        send(v.at[0, X - 1], hvx.at[0, 0], 0, 1),
        send(g.at[0, X - 1], hvx.at[0, 1], 0, 1),
        send(v.at[0, 0], hvx.at[1, 0], 0, -1),
        send(g.at[0, 0], hvx.at[1, 1], 0, -1),
    ]
    def send_x(part):
        return [
            send(nodes.at[1, part], nodes.at[X + 1, part], 0, -1),
            send(nodes.at[X, part], nodes.at[0, part], 0, 1),
        ]

    def send_y(start, size):
        rows = pl.ds(8 * start, 8 * size)
        return [
            send(y_s.at[0, :, rows], y_r.at[0, :, rows], 1, 1),
            send(y_s.at[1, :, rows], y_r.at[1, :, rows], 1, -1),
        ]

    for place in line:
        pl.semaphore_signal(
            plane_sem, inc=1, device_id=place, device_id_type=pl.DeviceIdType.MESH
        )

    def fold(value):
        value = functools.reduce(
            jnp.add, [value[i : i + SUBLANES, :] for i in range(0, value.shape[0], SUBLANES)]
        )
        return functools.reduce(
            jnp.add, [value[:, i : i + LANES] for i in range(0, value.shape[1], LANES)]
        )

    solve(edge, state, SWEEPS - EARLY_SWEEPS)
    y_copies = send_y(0, len(edge))
    x_copies = send_x(pl.ds(0, EARLY_NODES))

    for x in inner:
        loads[x].wait()
    if inner:
        solve(inner, start(inner, 0), SWEEPS)
        y_copies += send_y(len(edge), len(inner))
    wide_row = lax.broadcasted_iota(jnp.int32, (Y, Z), 0)
    wide_lane = lax.broadcasted_iota(jnp.int32, (Y, Z), 1)
    for x in range(X):
        for part, ref in ((0, v), (1, g)):
            half = 0.5 * ref[1, x]
            yu[x, part] = jnp.where(wide_row == Y - 1, 0.0, half + pltpu.roll(half, Y - 1, 0))
            yu[x, 2 + part] = jnp.where(wide_row == 0, 0.0, half + pltpu.roll(half, 1, 0))
            half = 0.5 * ref[2, x]
            zu[x, part] = jnp.where(wide_lane == Z - 1, 0.0, half + pltpu.roll(half, Z - 1, 1))
            zu[x, 2 + part] = jnp.where(wide_lane == 0, 0.0, half + pltpu.roll(half, 1, 1))
    for side in range(2):
        z_s[side] = columns[side]
    z_copies = [send(z_s.at[0], z_r.at[0], 2, 1), send(z_s.at[1], z_r.at[1], 2, -1)]
    m_sums = [functools.reduce(jnp.add, [fold(m[k, x]) for x in range(X)]) for k in range(8)]
    best = functools.reduce(jnp.maximum, [fastest(x) for x in range(X)])

    def lanes_of(chunk):
        return pl.ds(pl.multiple_of(chunk * LANES, LANES), LANES)

    def nodes_of(layer, zs, ys=slice(None)):
        return (
            [nodes[layer, i, ys, zs] for i in range(4)],
            [nodes[layer, 4 + i, ys, zs] for i in range(4)],
        )

    for copy in velocity_copies[:4]:
        copy.wait_recv()

    upwinds = (jnp.maximum, jnp.minimum)

    def y_mean(side):
        return [0.5 * (vy_s[side, part] + vy_r[1 - side, part]) for part in range(2)]

    def y_outflow(source, side, upwind, mean):
        rows = [
            jnp.concatenate([source[side, c, pl.ds(i, X, stride=8), :] for c in range(zc)], axis=1)
            for i in range(8)
        ]
        return outflow(rows[:4], rows[4:], *mean, upwind)

    def z_mean(side):
        mean = 0.5 * (vz_s[side] + vz_r[1 - side])
        return [mean, pltpu.roll(mean, LANES - X, 1)]

    def z_outflow(source, side, upwind, mean):
        tile = source[side]
        parts = [tile] + [pltpu.roll(tile, LANES - i * X, 1) for i in range(1, 8)]
        return outflow(parts[:4], parts[4:], *mean, upwind)

    y_sums = [y_outflow(y_s, side, upwinds[side], y_mean(side)) for side in range(2)]
    z_sums = [
        [
            jnp.where((lane < X) & jnp.logical_not((top, bottom)[side]), value, 0.0)
            for value in z_outflow(z_s, side, upwinds[side], z_mean(side))
        ]
        for side in range(2)
    ]

    for side in range(2):
        for k in range(8):
            y_face[1 - side, k] = y_sums[side][k]
            z_face[1 - side, k] = z_sums[side][k]

    for copy in velocity_copies[4:]:
        copy.wait_recv()

    def drift_of(x, zs):
        return v[0, x, :, zs], g[0, x, :, zs]

    def between(left, right):
        return 0.5 * (left[0] + right[0]), 0.5 * (left[1] + right[1])

    def side_x(i, sums):
        zs = lanes_of(i)
        ahead = between((hvx[0, 0, :, zs], hvx[0, 1, :, zs]), drift_of(0, zs))
        after = between(drift_of(X - 1, zs), (hvx[1, 0, :, zs], hvx[1, 1, :, zs]))
        upper = outflow(*nodes_of(X, zs), *after, jnp.maximum)
        lower = outflow(*nodes_of(1, zs), *ahead, jnp.minimum)
        for k in range(8):
            fx[X, k, :, zs] = upper[k]
            fx[0, k, :, zs] = lower[k]
        return tuple(a + fold(b) for a, b in zip(sums, upper + lower))

    zero = jnp.zeros((SUBLANES, LANES), jnp.float32)
    x_sums = lax.fori_loop(0, zc, side_x, (zero,) * 16)

    tile_row = lax.broadcasted_iota(jnp.int32, (SUBLANES, LANES), 0)
    tile_lane = lax.broadcasted_iota(jnp.int32, (SUBLANES, LANES), 1)

    def narrow(value):
        return functools.reduce(
            jnp.add, [value[:, i : i + LANES] for i in range(0, value.shape[1], LANES)]
        )

    packed = zero
    groups = [m_sums, x_sums[:8], x_sums[8:]] + [[narrow(a) for a in y] for y in y_sums] + z_sums
    for n, sums in enumerate(groups):
        block = zero
        for k in range(8):
            block = jnp.where(tile_row == k, jnp.sum(sums[k], axis=0, keepdims=True), block)
        value = jnp.sum(block, axis=1, keepdims=True)
        packed = jnp.where(tile_lane == tile_row + 8 * (n + 1), value, packed)
    packed = jnp.sum(packed, axis=0, keepdims=True)
    best = functools.reduce(
        jnp.maximum,
        [best[i : i + SUBLANES, j : j + LANES]
         for i in range(0, Y, SUBLANES) for j in range(0, Z, LANES)],
    )
    best = jnp.max(jnp.max(best, axis=0, keepdims=True), axis=1, keepdims=True)
    one_lane = lax.broadcasted_iota(jnp.int32, (1, LANES), 1)
    table[me] = jnp.where(one_lane == 0, best, packed)

    pl.semaphore_wait(plane_sem, len(line))

    def spread(j, carry):
        place = jnp.where(j >= me, j + 1, j)
        pltpu.make_async_remote_copy(
            src_ref=table.at[me], dst_ref=table.at[me],
            send_sem=all_sem.at[0], recv_sem=all_sem.at[1],
            device_id=place, device_id_type=pl.DeviceIdType.LOGICAL,
        ).start()
        return carry

    lax.fori_loop(0, count - 1, spread, 0)
    x_copies += send_x(pl.ds(EARLY_NODES, 8 - EARLY_NODES))

    def side_faces(i, carry):
        x, chunk = lax.div(i, zc), lax.rem(i, zc)
        zs = lanes_of(chunk)
        w, s = nodes_of(x + 1, zs)
        high = outflow(w, s, yu[x, 0, :, zs], yu[x, 1, :, zs], jnp.maximum)
        for k in range(8):
            acc[x, k, :, zs] = high[k] - jnp.where(row == 0, 0.0, pltpu.roll(high[k], 1, 0))
        low = outflow(w, s, yu[x, 2, :, zs], yu[x, 3, :, zs], jnp.minimum)
        for k in range(8):
            acc[x, k, :, zs] += (
                jnp.where(row == Y - 1, 0.0, pltpu.roll(low[k], Y - 1, 0)) - low[k]
            )
        return carry

    lax.fori_loop(0, X * zc, side_faces, 0)

    def wall_faces(i, carry):
        x, chunk = lax.div(i, zc), lax.rem(i, zc)
        zs = lanes_of(chunk)
        w, s = nodes_of(x + 1, zs)
        high = outflow(w, s, zu[x, 0, :, zs], zu[x, 1, :, zs], jnp.maximum)
        for k in range(8):
            zp[x, k, :, zs] = pltpu.roll(high[k], 1, 1)
        low = outflow(w, s, zu[x, 2, :, zs], zu[x, 3, :, zs], jnp.minimum)
        for k in range(8):
            zm[x, k, :, zs] = pltpu.roll(low[k], LANES - 1, 1)
            acc[x, k, :, zs] += high[k] - low[k]
        return carry

    lax.fori_loop(0, X * zc, wall_faces, 0)

    def face_x(face, zs, left, right):
        mean = between(left, right)
        upper = outflow(*nodes_of(face, zs), *mean, jnp.maximum)
        lower = outflow(*nodes_of(face + 1, zs), *mean, jnp.minimum)
        for k in range(8):
            fx[face, k, :, zs] = upper[k] + lower[k]

    def inner_x(i, carry):
        face, zs = lax.div(i, zc) + 1, lanes_of(lax.rem(i, zc))
        face_x(face, zs, drift_of(face - 1, zs), drift_of(face, zs))
        return carry

    def outer_x(i, carry):
        zs = lanes_of(i)
        ahead = between((hvx[0, 0, :, zs], hvx[0, 1, :, zs]), drift_of(0, zs))
        upper = outflow(*nodes_of(0, zs), *ahead, jnp.maximum)
        for k in range(8):
            acc[0, k, :, zs] -= upper[k]
        after = between(drift_of(X - 1, zs), (hvx[1, 0, :, zs], hvx[1, 1, :, zs]))
        lower = outflow(*nodes_of(X + 1, zs), *after, jnp.minimum)
        for k in range(8):
            acc[X - 1, k, :, zs] += lower[k]
        return carry

    if X > 1:
        lax.fori_loop(0, (X - 1) * zc, inner_x, 0)

    for copy in y_copies + z_copies:
        copy.wait_recv()
    for side in range(2):
        into = y_outflow(y_r, side, upwinds[side], y_mean(1 - side))
        for k in range(8):
            y_face[side, k] += into[k]
        into = z_outflow(z_r, side, upwinds[side], z_mean(1 - side))
        for k in range(8):
            z_face[side, k] += jnp.where((bottom, top)[side], 0.0, into[k])

    def combine(x, carry):
        p = jnp.where(x == 0, 0, jnp.where(x == X - 1, 1, x + 1))
        for k in range(8):
            floor, ceiling = y_face[0, k, pl.ds(p, 1), :], y_face[1, k, pl.ds(p, 1), :]
            first = pltpu.roll(z_face[0, k], lax.rem(LANES - p, LANES), 1)
            last = pltpu.roll(z_face[1, k], LANES - 1 - p, 1)
            rises = [zp[x, k, :, c * LANES : (c + 1) * LANES] for c in range(zc)]
            falls = [zm[x, k, :, c * LANES : (c + 1) * LANES] for c in range(zc)]
            for c in range(zc):
                zs = slice(c * LANES, (c + 1) * LANES)
                before = jnp.where(lane == 0, rises[c - 1] if c else first, rises[c])
                after = jnp.where(lane == LANES - 1, falls[c + 1] if c < zc - 1 else last, falls[c])
                change = acc[x, k, :, zs] + (after - before)
                change = change + (fx[x + 1, k, :, zs] - fx[x, k, :, zs])
                acc[x, k, :, zs] = change + jnp.where(
                    row == Y - 1, ceiling[:, zs], jnp.where(row == 0, -floor[:, zs], 0.0)
                )
        return carry

    lax.fori_loop(0, X, combine, 0)
    for copy in x_copies:
        copy.wait_recv()
    lax.fori_loop(0, zc, outer_x, 0)

    every = pltpu.make_async_copy(
        table.at[pl.ds(0, count - 1)], table.at[pl.ds(0, count - 1)], all_sem.at[1]
    )
    every.wait()
    rows = table[...]
    largest = jnp.max(jnp.max(rows, axis=0)[:, 0:1], axis=1, keepdims=True)
    step = jnp.broadcast_to(cfl_number / (largest + speed_eps), (Y, LANES))

    def update(x, carry):
        for k in range(8):
            for c in range(zc):
                zs = slice(c * LANES, (c + 1) * LANES)
                out[k, x, :, zs] = m[k, x, :, zs] - step * acc[x, k, :, zs]
        return carry

    lax.fori_loop(0, X, update, 0)

    grid = rows.reshape(sizes + (1, LANES))

    def turned(axis, step):
        size = sizes[axis]
        cut = (size - step) % size
        if cut == 0:
            return grid
        return jnp.concatenate(
            [lax.slice_in_dim(grid, cut, size, axis=axis), lax.slice_in_dim(grid, 0, cut, axis=axis)],
            axis=axis,
        )

    group = one_lane // 8
    net = jnp.zeros((1, LANES), jnp.float32)
    for axis in range(3):
        rise = jnp.sum((grid - turned(axis, 1)).reshape(count, 1, LANES), axis=0)
        fall = jnp.sum((turned(axis, -1) - grid).reshape(count, 1, LANES), axis=0)
        net = net + jnp.where(group == 2 + 2 * axis, rise, jnp.where(group == 3 + 2 * axis, fall, 0.0))
    net = jnp.broadcast_to(net, (SUBLANES, LANES))
    change = functools.reduce(jnp.add, [pltpu.roll(net, LANES - 8 * n, 1) for n in range(2, 8)])[0:1]
    both = pltpu.roll(jnp.broadcast_to(jnp.sum(rows, axis=0), (SUBLANES, LANES)), LANES - 8, 1)[0:1]
    tot_ref[...] = (both - step[0:1] * change) / float(count * X * Y * Z)

    for copy in sent:
        copy.wait_send()
    pltpu.make_async_copy(
        table.at[pl.ds(0, count - 1)], table.at[pl.ds(0, count - 1)], all_sem.at[0]
    ).wait()


def shards(sizes, moments, velocity, drift):
    _, X, Y, Z = moments.shape
    count = sizes[0] * sizes[1] * sizes[2]
    f32 = jnp.float32
    vm = lambda *shape: pltpu.VMEM(shape, f32)
    updated, totals = pl.pallas_call(
        functools.partial(kernel, sizes),
        name="transport",
        out_shape=(
            pltpu.VMEM(moments.shape, f32), pltpu.VMEM((1, LANES), f32)
        ),
        in_specs=[pl.BlockSpec(memory_space=pl.ANY)] * 3,
        out_specs=(
            pl.BlockSpec(memory_space=pltpu.VMEM), pl.BlockSpec(memory_space=pltpu.VMEM)
        ),
        scratch_shapes=[
            vm(8, X, Y, Z), vm(3, X, Y, Z), vm(3, X, Y, Z), vm(X + 2, 8, Y, Z), vm(X, 8, Y, Z),
            vm(X + 1, 8, Y, Z), vm(X, 8, Y, Z), vm(X, 8, Y, Z), vm(X, 4, Y, Z), vm(X, 4, Y, Z),
            vm(2, 2, Y, Z), vm(2, 2, X, Z), vm(2, 2, X, Z), vm(2, Y, LANES), vm(2, Y, LANES),
            vm(2, Z // LANES, 8 * X, LANES), vm(2, Z // LANES, 8 * X, LANES), vm(2, Y, LANES), vm(2, Y, LANES),
            vm(2, 8, X, Z), vm(2, 8, Y, LANES), vm(count, 1, LANES),
            pltpu.SemaphoreType.DMA((X + 2,)),
            pltpu.SemaphoreType.DMA((18,)), pltpu.SemaphoreType.DMA((18,)),
            pltpu.SemaphoreType.DMA((2,)), pltpu.SemaphoreType.REGULAR,
        ],
        compiler_params=pltpu.CompilerParams(
            collective_id=0, has_side_effects=True,
        ),
    )(moments, velocity, drift)
    return updated, totals[0, :8]


def solution(mesh):
    spec = P(None, "gx", "gy", "gz")
    sizes = tuple(mesh.shape[a] for a in AXES)
    return jax.shard_map(
        functools.partial(shards, sizes), mesh=mesh, in_specs=(spec,) * 3,
        out_specs=(spec, P()), check_vma=False,
    )
```

```python
import functools

import jax
import jax.numpy as jnp
from jax import lax
from jax.experimental import pallas as pl
from jax.experimental.pallas import tpu as pltpu
from jax.sharding import PartitionSpec as P

SWEEPS = 6
EARLY_NODES = 4
AXES = ("gx", "gy", "gz")
LANES = 128
SUBLANES = 8

cfl_number = 0.4
speed_eps = 1e-06
pair_list = ((0, 1), (0, 2), (0, 3), (1, 2), (1, 3), (2, 3))


def entry_key(i, j):
    return (min(i, j), max(i, j))


def scaled(scale, value):
    return value if scale is None else scale * value


def sheared(alpha, beta, near, far):
    if near is None and far is None:
        return None, None
    if near is None:
        return -(alpha * far), far
    if far is None:
        return near, beta * near
    return near - alpha * far, far + beta * near


def recurrence(moment):
    levels = list(moment)
    before = None
    inverse = 1.0 / levels[0]
    ratios = [levels[1] * inverse]
    alphas = [ratios[0]]
    betas = [levels[0]]
    for level in range(1, 4):
        fresh = [None] * 8
        for column in range(level, 8 - level):
            value = levels[column + 1] - alphas[level - 1] * levels[column]
            if level > 1:
                value = value - betas[level - 1] * before[column]
            fresh[column] = value
        betas.append(fresh[level] * inverse)
        inverse = 1.0 / fresh[level]
        ratios.append(fresh[level + 1] * inverse)
        alphas.append(ratios[level] - ratios[level - 1])
        before, levels = levels, fresh
    return alphas, betas


def begin(moment):
    diag, betas = recurrence(moment)
    table = {(i, j): None for i in range(4) for j in range(i + 1, 4)}
    for i in range(3):
        table[i, i + 1] = 2.0
    scale = [None, betas[1]]
    for i in range(2, 4):
        scale.append(betas[i] / scale[i - 1])
    return diag, table, scale, [1.0, None, None, None]


def sweep(state, sweeps):
    diag, table, scale, first = state
    for _ in range(sweeps):
        for p, q in pair_list:
            entry = table[p, q]
            if entry is None:
                continue
            spread = diag[q] - diag[p]
            left = scaled(scale[p], entry)
            right = scaled(scale[q], entry)
            r = lax.rsqrt(spread * spread + left * right)
            r = jnp.where(spread >= 0, r, -r)
            wide = 1.0 + spread * r
            turn = r / wide
            alpha = right * turn
            beta = left * turn
            shift = 0.5 * (left * alpha)
            half = 0.5 * wide
            scale[p] = scaled(scale[p], half)
            scale[q] = scaled(scale[q], half)
            for rest in range(4):
                if rest not in (p, q):
                    a, b = entry_key(rest, p), entry_key(rest, q)
                    table[a], table[b] = sheared(alpha, beta, table[a], table[b])
            diag[p] = diag[p] - shift
            diag[q] = diag[q] + shift
            table[p, q] = None
            first[p], first[q] = sheared(alpha, beta, first[p], first[q])


def quadrature(number, state):
    diag, table, scale, first = state
    return [number * (scale[i] * (first[i] * first[i])) for i in range(4)], diag


def outflow(weights, sizes, mean_speed, mean_drift, upwind):
    sums = None
    for w, s in zip(weights, sizes):
        term = w * upwind(mean_speed + mean_drift * s, 0.0)
        terms = [term]
        for _ in range(7):
            term = term * s
            terms.append(term)
        sums = terms if sums is None else [a + b for a, b in zip(sums, terms)]
    return sums


def kernel(
    sizes, m_hbm, v_hbm, g_hbm, acc, m, table,
    v, g, nodes, fx, zp, zm, yu, zu,
    hvx, vy_s, vy_r, vz_s, vz_r, y_s, y_r, z_s, z_r, y_face, z_face, tally,
    in_sem, nb_send, nb_recv, all_sem, plane_sem,
):
    X, Y, Z = m.shape[1:]
    count = sizes[0] * sizes[1] * sizes[2]
    zc = Z // LANES
    at = [lax.axis_index(a) for a in AXES]
    me = (at[0] * sizes[1] + at[1]) * sizes[2] + at[2]
    row = lax.broadcasted_iota(jnp.int32, (Y, LANES), 0)
    lane = lax.broadcasted_iota(jnp.int32, (Y, LANES), 1)
    bottom = at[2] == 0
    top = at[2] == sizes[2] - 1

    def along(axis, step):
        return lax.rem(at[axis] + step + sizes[axis], sizes[axis])

    def beside(axis, step):
        place = list(at)
        place[axis] = along(axis, step)
        return tuple(place)

    edge = [0] if X == 1 else [0, X - 1]
    inner = list(range(1, X - 1))

    def await_values(sem, number):
        rows = tally.at[pl.ds(0, number // LANES)]
        pltpu.make_async_copy(rows, rows, sem).wait()

    def load(layers, sem):
        for x in layers:
            for k in range(8):
                pltpu.make_async_copy(m_hbm.at[k, x], m.at[k, x], sem).start()
        return 8 * len(layers) * Y * Z

    first_load = load(edge, in_sem.at[0])
    for far, ref in ((v_hbm, v), (g_hbm, g)):
        for d in range(3):
            pltpu.make_async_copy(far.at[d], ref.at[d], in_sem.at[1]).start()
    second_load = load(inner, in_sem.at[1]) + 6 * X * Y * Z

    barrier = pltpu.get_barrier_semaphore()
    xs = [along(0, i) for i in range(sizes[0])]
    zs_ = [along(2, i) for i in range(sizes[2])]
    plane = [
        (xs[i], at[1], zs_[j]) for i in range(sizes[0]) for j in range(sizes[2]) if i or j
    ]
    line = [(at[0], along(1, i), at[2]) for i in range(1, sizes[1])]
    for place in plane + line:
        pl.semaphore_signal(
            barrier, inc=1, device_id=place, device_id_type=pl.DeviceIdType.MESH
        )

    V_SIDES, V_X, NODES_X, NODES_SIDES = range(4)
    sent, due = [0], [0] * 4

    def send(src, dst, axis, step, group):
        pltpu.make_async_remote_copy(
            src_ref=src, dst_ref=dst, send_sem=nb_send.at[0], recv_sem=nb_recv.at[group],
            device_id=beside(axis, step), device_id_type=pl.DeviceIdType.MESH,
        ).start()
        number = functools.reduce(lambda p, q: p * q, src.shape, 1)
        sent[0] += number
        due[group] += number

    def await_group(group):
        await_values(nb_recv.at[group], due[group])

    order = edge + inner
    columns = [jnp.zeros((Y, LANES), jnp.float32)] * 2

    def moments_of(layers, k):
        return jnp.concatenate([m[k, x] for x in layers], axis=0)

    def start(layers):
        return begin([moments_of(layers, k) for k in range(8)])

    def solve(layers, state):
        sweep(state, SWEEPS)
        weights, places = quadrature(moments_of(layers, 0), state)
        for n, x in enumerate(layers):
            for i in range(4):
                nodes[x + 1, i] = weights[i][n * Y : (n + 1) * Y]
                nodes[x + 1, 4 + i] = places[i][n * Y : (n + 1) * Y]
            for i, value in enumerate(weights + places):
                value = value[n * Y : (n + 1) * Y]
                p = order.index(x)
                for c in range(zc):
                    part = value[:, c * LANES : (c + 1) * LANES]
                    y_s[0, c, 8 * p + i : 8 * p + i + 1, :] = part[Y - 1 : Y]
                    y_s[1, c, 8 * p + i : 8 * p + i + 1, :] = part[0:1]
                spot = i * X + p
                for side, edge_lane in ((0, LANES - 1), (1, 0)):
                    tile = value[:, Z - LANES : Z] if side == 0 else value[:, 0:LANES]
                    turn = (spot - edge_lane) % LANES
                    tile = pltpu.roll(tile, turn, 1) if turn else tile
                    columns[side] = jnp.where(lane == spot, tile, columns[side])

    def fastest(x):
        speed = None
        for d in range(3):
            vd, gd = v[d, x], g[d, x]
            parts = [jnp.abs(vd + gd * nodes[x + 1, 4 + i]) for i in range(4)]
            largest = jnp.maximum(
                jnp.maximum(parts[0], parts[1]), jnp.maximum(parts[2], parts[3])
            )
            speed = largest if speed is None else speed + largest
        return speed

    await_values(in_sem.at[0], first_load)
    solve(edge, start(edge))
    await_values(in_sem.at[1], second_load)
    packs = [jnp.zeros((Y, LANES), jnp.float32)] * 2
    for p, x in enumerate(order):
        for part, ref in ((0, v), (1, g)):
            vy_s[0, part, p : p + 1, :] = ref[1, x, Y - 1 : Y, :]
            vy_s[1, part, p : p + 1, :] = ref[1, x, 0:1, :]
            spot = part * X + p
            tile = pltpu.roll(ref[2, x, :, Z - LANES : Z], spot + 1, 1)
            packs[0] = jnp.where(lane == spot, tile, packs[0])
            tile = ref[2, x, :, 0:LANES]
            tile = pltpu.roll(tile, spot, 1) if spot else tile
            packs[1] = jnp.where(lane == spot, tile, packs[1])
    for side in range(2):
        vz_s[side] = packs[side]
    pl.semaphore_wait(barrier, len(plane) + len(line))
    for side, step in ((0, 1), (1, -1)):
        send(vy_s.at[side], vy_r.at[side], 1, step, V_SIDES)
        send(vz_s.at[side], vz_r.at[side], 2, step, V_SIDES)
    for side, step, x in ((0, 1, X - 1), (1, -1, 0)):
        send(v.at[0, x], hvx.at[side, 0], 0, step, V_X)
        send(g.at[0, x], hvx.at[side, 1], 0, step, V_X)

    def send_x(part):
        send(nodes.at[1, part], nodes.at[X + 1, part], 0, -1, NODES_X)
        send(nodes.at[X, part], nodes.at[0, part], 0, 1, NODES_X)

    def send_y(start, size):
        rows = pl.ds(8 * start, 8 * size)
        send(y_s.at[0, :, rows], y_r.at[0, :, rows], 1, 1, NODES_SIDES)
        send(y_s.at[1, :, rows], y_r.at[1, :, rows], 1, -1, NODES_SIDES)

    for place in line:
        pl.semaphore_signal(
            plane_sem, inc=1, device_id=place, device_id_type=pl.DeviceIdType.MESH
        )

    def fold(value):
        value = functools.reduce(
            jnp.add, [value[i : i + SUBLANES, :] for i in range(0, value.shape[0], SUBLANES)]
        )
        return functools.reduce(
            jnp.add, [value[:, i : i + LANES] for i in range(0, value.shape[1], LANES)]
        )

    send_y(0, len(edge))
    send_x(pl.ds(0, EARLY_NODES))

    if inner:
        solve(inner, start(inner))
        send_y(len(edge), len(inner))
    wide_row = lax.broadcasted_iota(jnp.int32, (Y, Z), 0)
    wide_lane = lax.broadcasted_iota(jnp.int32, (Y, Z), 1)
    for x in range(X):
        for part, ref in ((0, v), (1, g)):
            half = 0.5 * ref[1, x]
            yu[x, part] = jnp.where(wide_row == Y - 1, 0.0, half + pltpu.roll(half, Y - 1, 0))
            yu[x, 2 + part] = jnp.where(wide_row == 0, 0.0, half + pltpu.roll(half, 1, 0))
            half = 0.5 * ref[2, x]
            zu[x, part] = jnp.where(wide_lane == Z - 1, 0.0, half + pltpu.roll(half, Z - 1, 1))
            zu[x, 2 + part] = jnp.where(wide_lane == 0, 0.0, half + pltpu.roll(half, 1, 1))
    for side in range(2):
        z_s[side] = columns[side]
    for side, step in ((0, 1), (1, -1)):
        send(z_s.at[side], z_r.at[side], 2, step, NODES_SIDES)
    m_sums = [functools.reduce(jnp.add, [fold(m[k, x]) for x in range(X)]) for k in range(8)]
    best = functools.reduce(jnp.maximum, [fastest(x) for x in range(X)])

    def lanes_of(chunk):
        return pl.ds(pl.multiple_of(chunk * LANES, LANES), LANES)

    def nodes_of(layer, zs, ys=slice(None)):
        return (
            [nodes[layer, i, ys, zs] for i in range(4)],
            [nodes[layer, 4 + i, ys, zs] for i in range(4)],
        )

    await_group(V_SIDES)

    upwinds = (jnp.maximum, jnp.minimum)

    def y_mean(side):
        return [0.5 * (vy_s[side, part] + vy_r[1 - side, part]) for part in range(2)]

    def y_outflow(source, side, upwind, mean):
        rows = [
            jnp.concatenate([source[side, c, pl.ds(i, X, stride=8), :] for c in range(zc)], axis=1)
            for i in range(8)
        ]
        return outflow(rows[:4], rows[4:], *mean, upwind)

    def z_mean(side):
        mean = 0.5 * (vz_s[side] + vz_r[1 - side])
        return [mean, pltpu.roll(mean, LANES - X, 1)]

    def z_outflow(source, side, upwind, mean):
        tile = source[side]
        parts = [tile] + [pltpu.roll(tile, LANES - i * X, 1) for i in range(1, 8)]
        return outflow(parts[:4], parts[4:], *mean, upwind)

    y_sums = [y_outflow(y_s, side, upwinds[side], y_mean(side)) for side in range(2)]
    z_sums = [
        [
            jnp.where((lane < X) & jnp.logical_not((top, bottom)[side]), value, 0.0)
            for value in z_outflow(z_s, side, upwinds[side], z_mean(side))
        ]
        for side in range(2)
    ]

    for side in range(2):
        for k in range(8):
            y_face[1 - side, k] = y_sums[side][k]
            z_face[1 - side, k] = z_sums[side][k]

    await_group(V_X)

    def drift_of(x, zs):
        return v[0, x, :, zs], g[0, x, :, zs]

    def between(left, right):
        return 0.5 * (left[0] + right[0]), 0.5 * (left[1] + right[1])

    def side_x(i, sums):
        zs = lanes_of(i)
        ahead = between((hvx[0, 0, :, zs], hvx[0, 1, :, zs]), drift_of(0, zs))
        after = between(drift_of(X - 1, zs), (hvx[1, 0, :, zs], hvx[1, 1, :, zs]))
        upper = outflow(*nodes_of(X, zs), *after, jnp.maximum)
        lower = outflow(*nodes_of(1, zs), *ahead, jnp.minimum)
        for k in range(8):
            fx[X, k, :, zs] = upper[k]
            fx[0, k, :, zs] = lower[k]
        return tuple(a + fold(b) for a, b in zip(sums, upper + lower))

    zero = jnp.zeros((SUBLANES, LANES), jnp.float32)
    x_sums = lax.fori_loop(0, zc, side_x, (zero,) * 16)

    tile_row = lax.broadcasted_iota(jnp.int32, (SUBLANES, LANES), 0)
    tile_lane = lax.broadcasted_iota(jnp.int32, (SUBLANES, LANES), 1)

    def narrow(value):
        return functools.reduce(
            jnp.add, [value[:, i : i + LANES] for i in range(0, value.shape[1], LANES)]
        )

    packed = zero
    groups = [m_sums, x_sums[:8], x_sums[8:]] + [[narrow(a) for a in y] for y in y_sums] + z_sums
    for n, sums in enumerate(groups):
        block = zero
        for k in range(8):
            block = jnp.where(tile_row == k, jnp.sum(sums[k], axis=0, keepdims=True), block)
        value = jnp.sum(block, axis=1, keepdims=True)
        packed = jnp.where(tile_lane == tile_row + 8 * n, value, packed)
    packed = jnp.sum(packed, axis=0, keepdims=True)
    best = functools.reduce(
        jnp.maximum,
        [best[i : i + SUBLANES, j : j + LANES]
         for i in range(0, Y, SUBLANES) for j in range(0, Z, LANES)],
    )
    best = jnp.max(jnp.max(best, axis=0, keepdims=True), axis=1, keepdims=True)
    table[me, 0:1] = jnp.broadcast_to(best, (1, LANES))
    table[me, 1:2] = packed

    pl.semaphore_wait(plane_sem, len(line))

    def spread(j, carry):
        place = jnp.where(j >= me, j + 1, j)
        pltpu.make_async_remote_copy(
            src_ref=table.at[me], dst_ref=table.at[me],
            send_sem=all_sem.at[0], recv_sem=all_sem.at[1],
            device_id=place, device_id_type=pl.DeviceIdType.LOGICAL,
        ).start()
        return carry

    lax.fori_loop(0, count - 1, spread, 0)
    send_x(pl.ds(EARLY_NODES, 8 - EARLY_NODES))

    def side_faces(i, carry):
        x, chunk = lax.div(i, zc), lax.rem(i, zc)
        zs = lanes_of(chunk)
        w, s = nodes_of(x + 1, zs)
        high = outflow(w, s, yu[x, 0, :, zs], yu[x, 1, :, zs], jnp.maximum)
        for k in range(8):
            acc[x, k, :, zs] = high[k] - jnp.where(row == 0, 0.0, pltpu.roll(high[k], 1, 0))
        low = outflow(w, s, yu[x, 2, :, zs], yu[x, 3, :, zs], jnp.minimum)
        for k in range(8):
            acc[x, k, :, zs] += (
                jnp.where(row == Y - 1, 0.0, pltpu.roll(low[k], Y - 1, 0)) - low[k]
            )
        return carry

    lax.fori_loop(0, X * zc, side_faces, 0)

    def wall_faces(i, carry):
        x, chunk = lax.div(i, zc), lax.rem(i, zc)
        zs = lanes_of(chunk)
        w, s = nodes_of(x + 1, zs)
        high = outflow(w, s, zu[x, 0, :, zs], zu[x, 1, :, zs], jnp.maximum)
        for k in range(8):
            zp[x, k, :, zs] = pltpu.roll(high[k], 1, 1)
        low = outflow(w, s, zu[x, 2, :, zs], zu[x, 3, :, zs], jnp.minimum)
        for k in range(8):
            zm[x, k, :, zs] = pltpu.roll(low[k], LANES - 1, 1)
            acc[x, k, :, zs] += high[k] - low[k]
        return carry

    lax.fori_loop(0, X * zc, wall_faces, 0)

    def face_x(face, zs, left, right):
        mean = between(left, right)
        upper = outflow(*nodes_of(face, zs), *mean, jnp.maximum)
        lower = outflow(*nodes_of(face + 1, zs), *mean, jnp.minimum)
        for k in range(8):
            fx[face, k, :, zs] = upper[k] + lower[k]

    def inner_x(i, carry):
        face, zs = lax.div(i, zc) + 1, lanes_of(lax.rem(i, zc))
        face_x(face, zs, drift_of(face - 1, zs), drift_of(face, zs))
        return carry

    def outer_x(i, carry):
        zs = lanes_of(i)
        ahead = between((hvx[0, 0, :, zs], hvx[0, 1, :, zs]), drift_of(0, zs))
        upper = outflow(*nodes_of(0, zs), *ahead, jnp.maximum)
        for k in range(8):
            acc[0, k, :, zs] -= upper[k]
        after = between(drift_of(X - 1, zs), (hvx[1, 0, :, zs], hvx[1, 1, :, zs]))
        lower = outflow(*nodes_of(X + 1, zs), *after, jnp.minimum)
        for k in range(8):
            acc[X - 1, k, :, zs] += lower[k]
        return carry

    if X > 1:
        lax.fori_loop(0, (X - 1) * zc, inner_x, 0)

    await_group(NODES_SIDES)
    for side in range(2):
        into = y_outflow(y_r, side, upwinds[side], y_mean(1 - side))
        for k in range(8):
            y_face[side, k] += into[k]
        into = z_outflow(z_r, side, upwinds[side], z_mean(1 - side))
        for k in range(8):
            z_face[side, k] += jnp.where((bottom, top)[side], 0.0, into[k])

    def combine(x, carry):
        p = jnp.where(x == 0, 0, jnp.where(x == X - 1, 1, x + 1))
        for k in range(8):
            floor, ceiling = y_face[0, k, pl.ds(p, 1), :], y_face[1, k, pl.ds(p, 1), :]
            first = pltpu.roll(z_face[0, k], lax.rem(LANES - p, LANES), 1)
            last = pltpu.roll(z_face[1, k], LANES - 1 - p, 1)
            rises = [zp[x, k, :, c * LANES : (c + 1) * LANES] for c in range(zc)]
            falls = [zm[x, k, :, c * LANES : (c + 1) * LANES] for c in range(zc)]
            for c in range(zc):
                zs = slice(c * LANES, (c + 1) * LANES)
                before = jnp.where(lane == 0, rises[c - 1] if c else first, rises[c])
                after = jnp.where(lane == LANES - 1, falls[c + 1] if c < zc - 1 else last, falls[c])
                change = acc[x, k, :, zs] + (after - before)
                change = change + (fx[x + 1, k, :, zs] - fx[x, k, :, zs])
                acc[x, k, :, zs] = change + jnp.where(
                    row == Y - 1, ceiling[:, zs], jnp.where(row == 0, -floor[:, zs], 0.0)
                )
        return carry

    lax.fori_loop(0, X, combine, 0)
    await_group(NODES_X)
    lax.fori_loop(0, zc, outer_x, 0)

    every = pltpu.make_async_copy(
        table.at[pl.ds(0, count - 1)], table.at[pl.ds(0, count - 1)], all_sem.at[1]
    )
    every.wait()
    await_values(nb_send.at[0], sent[0])
    pltpu.make_async_copy(
        table.at[pl.ds(0, count - 1)], table.at[pl.ds(0, count - 1)], all_sem.at[0]
    ).wait()


def finish(sizes, acc, m, table, out_hbm, tot_hbm, stage, tot, sem):
    X, Y, Z = m.shape[1:]
    count = sizes[0] * sizes[1] * sizes[2]
    largest = jnp.max(table[:, 0:1, :], axis=0)
    step = cfl_number / (jnp.broadcast_to(largest, (Y, LANES)) + speed_eps)
    copies = []
    for k in range(8):
        for x in range(X):
            for c in range(Z // LANES):
                zs = slice(c * LANES, (c + 1) * LANES)
                stage[k, x, :, zs] = m[k, x, :, zs] - step * acc[x, k, :, zs]
        copies.append(pltpu.make_async_copy(stage.at[k], out_hbm.at[k], sem.at[k]))
        copies[-1].start()

    rows = table[:, 1:2, :]
    grid = rows.reshape(sizes + (1, LANES))

    def turned(axis, step):
        size = sizes[axis]
        cut = (size - step) % size
        if cut == 0:
            return grid
        return jnp.concatenate(
            [lax.slice_in_dim(grid, cut, size, axis=axis), lax.slice_in_dim(grid, 0, cut, axis=axis)],
            axis=axis,
        )

    group = lax.broadcasted_iota(jnp.int32, (1, LANES), 1) // 8
    net = jnp.zeros((1, LANES), jnp.float32)
    for axis in range(3):
        rise = jnp.sum((grid - turned(axis, 1)).reshape(count, 1, LANES), axis=0)
        fall = jnp.sum((turned(axis, -1) - grid).reshape(count, 1, LANES), axis=0)
        net = net + jnp.where(
            group == 1 + 2 * axis, rise, jnp.where(group == 2 + 2 * axis, fall, 0.0)
        )
    net = jnp.broadcast_to(net, (SUBLANES, LANES))
    change = functools.reduce(jnp.add, [pltpu.roll(net, LANES - 8 * n, 1) for n in range(1, 7)])
    both = jnp.sum(rows, axis=0) - step[0:1] * change[0:1]
    tot[...] = (both / float(count * X * Y * Z))[:, 0:8].reshape(8)
    copies.append(pltpu.make_async_copy(tot, tot_hbm, sem.at[8]))
    copies[-1].start()
    for copy in copies:
        copy.wait()


def shards(sizes, moments, velocity, drift):
    _, X, Y, Z = moments.shape
    count = sizes[0] * sizes[1] * sizes[2]
    f32 = jnp.float32
    vm = lambda *shape: pltpu.VMEM(shape, f32)
    near = pl.BlockSpec(memory_space=pltpu.VMEM)
    far = pl.BlockSpec(memory_space=pl.ANY)
    parts = pl.pallas_call(
        functools.partial(kernel, sizes),
        name="transport",
        out_shape=(vm(X, 8, Y, Z), vm(*moments.shape), vm(count, 2, LANES)),
        in_specs=[far] * 3,
        out_specs=(near,) * 3,
        scratch_shapes=[
            vm(3, X, Y, Z), vm(3, X, Y, Z), vm(X + 2, 8, Y, Z),
            vm(X + 1, 8, Y, Z), vm(X, 8, Y, Z), vm(X, 8, Y, Z), vm(X, 4, Y, Z), vm(X, 4, Y, Z),
            vm(2, 2, Y, Z), vm(2, 2, X, Z), vm(2, 2, X, Z), vm(2, Y, LANES), vm(2, Y, LANES),
            vm(2, Z // LANES, 8 * X, LANES), vm(2, Z // LANES, 8 * X, LANES),
            vm(2, Y, LANES), vm(2, Y, LANES),
            vm(2, 8, X, Z), vm(2, 8, Y, LANES), vm(14 * X * Y * Z // LANES, LANES),
            pltpu.SemaphoreType.DMA((2,)), pltpu.SemaphoreType.DMA((1,)),
            pltpu.SemaphoreType.DMA((4,)), pltpu.SemaphoreType.DMA((2,)),
            pltpu.SemaphoreType.REGULAR,
        ],
        compiler_params=pltpu.CompilerParams(
            collective_id=0, has_side_effects=True,
        ),
    )(moments, velocity, drift)
    return pl.pallas_call(
        functools.partial(finish, sizes),
        name="finish",
        out_shape=(jax.ShapeDtypeStruct(moments.shape, f32), jax.ShapeDtypeStruct((8,), f32)),
        in_specs=[near] * 3,
        out_specs=(far, far),
        scratch_shapes=[vm(*moments.shape), vm(8), pltpu.SemaphoreType.DMA((9,))],
    )(*(pltpu.with_memory_space_constraint(part, pltpu.VMEM) for part in parts))


def solution(mesh):
    spec = P(None, "gx", "gy", "gz")
    sizes = tuple(mesh.shape[a] for a in AXES)
    return jax.shard_map(
        functools.partial(shards, sizes), mesh=mesh, in_specs=(spec,) * 3,
        out_specs=(spec, P()), check_vma=False,
    )
```

```python
import functools

import jax
import jax.numpy as jnp
from jax import lax
from jax.experimental import pallas as pl
from jax.experimental.pallas import tpu as pltpu
from jax.sharding import PartitionSpec as P

SWEEPS = 6
EARLY_NODES = 4
AXES = ("gx", "gy", "gz")
LANES = 128
SUBLANES = 8

cfl_number = 0.4
speed_eps = 1e-06
pair_list = ((0, 1), (0, 2), (0, 3), (1, 2), (1, 3), (2, 3))


def entry_key(i, j):
    return (min(i, j), max(i, j))


def scaled(scale, value):
    return value if scale is None else scale * value


def sheared(alpha, beta, near, far):
    if near is None and far is None:
        return None, None
    if near is None:
        return -(alpha * far), far
    if far is None:
        return near, beta * near
    return near - alpha * far, far + beta * near


def recurrence(moment):
    levels = list(moment)
    before = None
    inverse = 1.0 / levels[0]
    ratios = [levels[1] * inverse]
    alphas = [ratios[0]]
    betas = [levels[0]]
    for level in range(1, 4):
        fresh = [None] * 8
        for column in range(level, 8 - level):
            value = levels[column + 1] - alphas[level - 1] * levels[column]
            if level > 1:
                value = value - betas[level - 1] * before[column]
            fresh[column] = value
        betas.append(fresh[level] * inverse)
        inverse = 1.0 / fresh[level]
        ratios.append(fresh[level + 1] * inverse)
        alphas.append(ratios[level] - ratios[level - 1])
        before, levels = levels, fresh
    return alphas, betas


def begin(moment):
    diag, betas = recurrence(moment)
    table = {(i, j): None for i in range(4) for j in range(i + 1, 4)}
    for i in range(3):
        table[i, i + 1] = 2.0
    scale = [None, betas[1]]
    for i in range(2, 4):
        scale.append(betas[i] / scale[i - 1])
    return diag, table, scale, [1.0, None, None, None]


def sweep(state, sweeps):
    diag, table, scale, first = state
    for _ in range(sweeps):
        for p, q in pair_list:
            entry = table[p, q]
            if entry is None:
                continue
            spread = diag[q] - diag[p]
            left = scaled(scale[p], entry)
            right = scaled(scale[q], entry)
            square = spread * spread + left * right
            r = lax.rsqrt(square)
            r = jnp.where(spread >= 0, r, -r)
            both = spread + square * r
            turn = 1.0 / both
            half = 0.5 * both
            alpha = right * turn
            beta = left * turn
            shrink = half * r
            scale[p] = scaled(scale[p], shrink)
            scale[q] = scaled(scale[q], shrink)
            for rest in range(4):
                if rest not in (p, q):
                    a, b = entry_key(rest, p), entry_key(rest, q)
                    table[a], table[b] = sheared(alpha, beta, table[a], table[b])
            diag[p], diag[q] = diag[q] - half, diag[p] + half
            table[p, q] = None
            first[p], first[q] = sheared(alpha, beta, first[p], first[q])


def quadrature(number, state):
    diag, table, scale, first = state
    return [number * (scale[i] * (first[i] * first[i])) for i in range(4)], diag


def outflow(weights, sizes, mean_speed, mean_drift, upwind):
    sums = None
    for w, s in zip(weights, sizes):
        term = w * upwind(mean_speed + mean_drift * s, 0.0)
        terms = [term]
        for _ in range(7):
            term = term * s
            terms.append(term)
        sums = terms if sums is None else [a + b for a, b in zip(sums, terms)]
    return sums


def kernel(
    sizes, m_hbm, v_hbm, g_hbm, acc, m, table,
    v, g, nodes, fx, zp, zm, yu, zu,
    hvx, vy_s, vy_r, vz_s, vz_r, y_s, y_r, z_s, z_r, y_face, z_face, tally,
    in_sem, nb_send, nb_recv, all_sem, plane_sem,
):
    X, Y, Z = m.shape[1:]
    count = sizes[0] * sizes[1] * sizes[2]
    zc = Z // LANES
    at = [lax.axis_index(a) for a in AXES]
    me = (at[0] * sizes[1] + at[1]) * sizes[2] + at[2]
    row = lax.broadcasted_iota(jnp.int32, (Y, LANES), 0)
    lane = lax.broadcasted_iota(jnp.int32, (Y, LANES), 1)
    bottom = at[2] == 0
    top = at[2] == sizes[2] - 1

    def along(axis, step):
        return lax.rem(at[axis] + step + sizes[axis], sizes[axis])

    def beside(axis, step):
        place = list(at)
        place[axis] = along(axis, step)
        return tuple(place)

    edge = [0] if X == 1 else [0, X - 1]
    inner = list(range(1, X - 1))

    def await_values(sem, number):
        rows = tally.at[pl.ds(0, number // LANES)]
        pltpu.make_async_copy(rows, rows, sem).wait()

    def load(layers, sem):
        for x in layers:
            for k in range(8):
                pltpu.make_async_copy(m_hbm.at[k, x], m.at[k, x], sem).start()
        return 8 * len(layers) * Y * Z

    first_load = load(edge, in_sem.at[0])
    for far, ref in ((v_hbm, v), (g_hbm, g)):
        for d in range(3):
            pltpu.make_async_copy(far.at[d], ref.at[d], in_sem.at[1]).start()
    second_load = load(inner, in_sem.at[1]) + 6 * X * Y * Z

    barrier = pltpu.get_barrier_semaphore()
    xs = [along(0, i) for i in range(sizes[0])]
    zs_ = [along(2, i) for i in range(sizes[2])]
    plane = [
        (xs[i], at[1], zs_[j]) for i in range(sizes[0]) for j in range(sizes[2]) if i or j
    ]
    line = [(at[0], along(1, i), at[2]) for i in range(1, sizes[1])]
    for place in plane + line:
        pl.semaphore_signal(
            barrier, inc=1, device_id=place, device_id_type=pl.DeviceIdType.MESH
        )

    V_SIDES, V_X, NODES_X, NODES_SIDES = range(4)
    sent, due = [0], [0] * 4

    def send(src, dst, axis, step, group, counted=True):
        pltpu.make_async_remote_copy(
            src_ref=src, dst_ref=dst, send_sem=nb_send.at[0], recv_sem=nb_recv.at[group],
            device_id=beside(axis, step), device_id_type=pl.DeviceIdType.MESH,
        ).start()
        number = functools.reduce(lambda p, q: p * q, src.shape, 1) if counted else 0
        sent[0] += number
        due[group] += number

    def await_group(group):
        await_values(nb_recv.at[group], due[group])

    order = edge + inner
    columns = [jnp.zeros((Y, LANES), jnp.float32)] * 2

    def moments_of(layers, k):
        return jnp.concatenate([m[k, x] for x in layers], axis=0)

    def start(layers):
        return begin([moments_of(layers, k) for k in range(8)])

    def solve(layers, state):
        sweep(state, SWEEPS)
        weights, places = quadrature(moments_of(layers, 0), state)
        for n, x in enumerate(layers):
            for i in range(4):
                nodes[x + 1, i] = weights[i][n * Y : (n + 1) * Y]
                nodes[x + 1, 4 + i] = places[i][n * Y : (n + 1) * Y]
            for i, value in enumerate(weights + places):
                value = value[n * Y : (n + 1) * Y]
                p = order.index(x)
                for c in range(zc):
                    part = value[:, c * LANES : (c + 1) * LANES]
                    y_s[0, c, 8 * p + i : 8 * p + i + 1, :] = part[Y - 1 : Y]
                    y_s[1, c, 8 * p + i : 8 * p + i + 1, :] = part[0:1]
                spot = i * X + p
                for side, edge_lane in ((0, LANES - 1), (1, 0)):
                    tile = value[:, Z - LANES : Z] if side == 0 else value[:, 0:LANES]
                    turn = (spot - edge_lane) % LANES
                    tile = pltpu.roll(tile, turn, 1) if turn else tile
                    columns[side] = jnp.where(lane == spot, tile, columns[side])

    def fastest(x):
        speed = None
        for d in range(3):
            vd, gd = v[d, x], g[d, x]
            parts = [jnp.abs(vd + gd * nodes[x + 1, 4 + i]) for i in range(4)]
            largest = jnp.maximum(
                jnp.maximum(parts[0], parts[1]), jnp.maximum(parts[2], parts[3])
            )
            speed = largest if speed is None else speed + largest
        return speed

    await_values(in_sem.at[0], first_load)
    solve(edge, start(edge))
    await_values(in_sem.at[1], second_load)
    packs = [jnp.zeros((Y, LANES), jnp.float32)] * 2
    for p, x in enumerate(order):
        for part, ref in ((0, v), (1, g)):
            vy_s[0, part, p : p + 1, :] = ref[1, x, Y - 1 : Y, :]
            vy_s[1, part, p : p + 1, :] = ref[1, x, 0:1, :]
            spot = part * X + p
            tile = pltpu.roll(ref[2, x, :, Z - LANES : Z], spot + 1, 1)
            packs[0] = jnp.where(lane == spot, tile, packs[0])
            tile = ref[2, x, :, 0:LANES]
            tile = pltpu.roll(tile, spot, 1) if spot else tile
            packs[1] = jnp.where(lane == spot, tile, packs[1])
    for side in range(2):
        vz_s[side] = packs[side]
    pl.semaphore_wait(barrier, len(plane) + len(line))
    for side, step in ((0, 1), (1, -1)):
        send(vy_s.at[side], vy_r.at[side], 1, step, V_SIDES)
        send(vz_s.at[side], vz_r.at[side], 2, step, V_SIDES)
    for side, step, x in ((0, 1, X - 1), (1, -1, 0)):
        send(v.at[0, x], hvx.at[side, 0], 0, step, V_X)
        send(g.at[0, x], hvx.at[side, 1], 0, step, V_X)

    def send_x(part, counted=True):
        send(nodes.at[1, part], nodes.at[X + 1, part], 0, -1, NODES_X, counted)
        send(nodes.at[X, part], nodes.at[0, part], 0, 1, NODES_X, counted)

    def send_y(start, size):
        rows = pl.ds(8 * start, 8 * size)
        send(y_s.at[0, :, rows], y_r.at[0, :, rows], 1, 1, NODES_SIDES)
        send(y_s.at[1, :, rows], y_r.at[1, :, rows], 1, -1, NODES_SIDES)

    for place in line:
        pl.semaphore_signal(
            plane_sem, inc=1, device_id=place, device_id_type=pl.DeviceIdType.MESH
        )

    def fold(value):
        value = functools.reduce(
            jnp.add, [value[i : i + SUBLANES, :] for i in range(0, value.shape[0], SUBLANES)]
        )
        return functools.reduce(
            jnp.add, [value[:, i : i + LANES] for i in range(0, value.shape[1], LANES)]
        )

    send_y(0, len(edge))
    send_x(pl.ds(0, EARLY_NODES))

    if inner:
        solve(inner, start(inner))
        send_y(len(edge), len(inner))
    for side in range(2):
        z_s[side] = columns[side]
    for side, step in ((0, 1), (1, -1)):
        send(z_s.at[side], z_r.at[side], 2, step, NODES_SIDES)
    m_sums = [functools.reduce(jnp.add, [fold(m[k, x]) for x in range(X)]) for k in range(8)]
    best = functools.reduce(jnp.maximum, [fastest(x) for x in range(X)])

    def lanes_of(chunk):
        return pl.ds(pl.multiple_of(chunk * LANES, LANES), LANES)

    def nodes_of(layer, zs, ys=slice(None)):
        return (
            [nodes[layer, i, ys, zs] for i in range(4)],
            [nodes[layer, 4 + i, ys, zs] for i in range(4)],
        )

    last_nodes = pl.ds(EARLY_NODES, 8 - EARLY_NODES)
    pl.when(at[1] == 0)(lambda: send_x(last_nodes))
    await_group(V_SIDES)

    upwinds = (jnp.maximum, jnp.minimum)

    def y_mean(side):
        return [0.5 * (vy_s[side, part] + vy_r[1 - side, part]) for part in range(2)]

    def y_outflow(source, side, upwind, mean):
        rows = [
            jnp.concatenate([source[side, c, pl.ds(i, X, stride=8), :] for c in range(zc)], axis=1)
            for i in range(8)
        ]
        return outflow(rows[:4], rows[4:], *mean, upwind)

    def z_mean(side):
        mean = 0.5 * (vz_s[side] + vz_r[1 - side])
        return [mean, pltpu.roll(mean, LANES - X, 1)]

    def z_outflow(source, side, upwind, mean):
        tile = source[side]
        parts = [tile] + [pltpu.roll(tile, LANES - i * X, 1) for i in range(1, 8)]
        return outflow(parts[:4], parts[4:], *mean, upwind)

    y_sums = [y_outflow(y_s, side, upwinds[side], y_mean(side)) for side in range(2)]
    z_sums = [
        [
            jnp.where((lane < X) & jnp.logical_not((top, bottom)[side]), value, 0.0)
            for value in z_outflow(z_s, side, upwinds[side], z_mean(side))
        ]
        for side in range(2)
    ]

    for side in range(2):
        for k in range(8):
            y_face[1 - side, k] = y_sums[side][k]
            z_face[1 - side, k] = z_sums[side][k]

    await_group(V_X)

    def drift_of(x, zs):
        return v[0, x, :, zs], g[0, x, :, zs]

    def between(left, right):
        return 0.5 * (left[0] + right[0]), 0.5 * (left[1] + right[1])

    def side_x(i, sums):
        zs = lanes_of(i)
        ahead = between((hvx[0, 0, :, zs], hvx[0, 1, :, zs]), drift_of(0, zs))
        after = between(drift_of(X - 1, zs), (hvx[1, 0, :, zs], hvx[1, 1, :, zs]))
        upper = outflow(*nodes_of(X, zs), *after, jnp.maximum)
        lower = outflow(*nodes_of(1, zs), *ahead, jnp.minimum)
        for k in range(8):
            fx[X, k, :, zs] = upper[k]
            fx[0, k, :, zs] = lower[k]
        return tuple(a + fold(b) for a, b in zip(sums, upper + lower))

    zero = jnp.zeros((SUBLANES, LANES), jnp.float32)
    x_sums = lax.fori_loop(0, zc, side_x, (zero,) * 16)

    tile_row = lax.broadcasted_iota(jnp.int32, (SUBLANES, LANES), 0)
    tile_lane = lax.broadcasted_iota(jnp.int32, (SUBLANES, LANES), 1)

    def narrow(value):
        return functools.reduce(
            jnp.add, [value[:, i : i + LANES] for i in range(0, value.shape[1], LANES)]
        )

    packed = zero
    groups = [m_sums, x_sums[:8], x_sums[8:]] + [[narrow(a) for a in y] for y in y_sums] + z_sums
    for n, sums in enumerate(groups):
        block = zero
        for k in range(8):
            block = jnp.where(tile_row == k, jnp.sum(sums[k], axis=0, keepdims=True), block)
        value = jnp.sum(block, axis=1, keepdims=True)
        packed = jnp.where(tile_lane == tile_row + 8 * n, value, packed)
    packed = jnp.sum(packed, axis=0, keepdims=True)
    best = functools.reduce(
        jnp.maximum,
        [best[i : i + SUBLANES, j : j + LANES]
         for i in range(0, Y, SUBLANES) for j in range(0, Z, LANES)],
    )
    best = jnp.max(jnp.max(best, axis=0, keepdims=True), axis=1, keepdims=True)
    table[me, 0:1] = jnp.broadcast_to(best, (1, LANES))
    table[me, 1:2] = packed

    pl.semaphore_wait(plane_sem, len(line))

    def spread(j, carry):
        place = jnp.where(j >= me, j + 1, j)
        pltpu.make_async_remote_copy(
            src_ref=table.at[me], dst_ref=table.at[me],
            send_sem=all_sem.at[0], recv_sem=all_sem.at[1],
            device_id=place, device_id_type=pl.DeviceIdType.LOGICAL,
        ).start()
        return carry

    lax.fori_loop(0, count - 1, spread, 0)
    pl.when(at[1] != 0)(lambda: send_x(last_nodes, False))

    wide_row = lax.broadcasted_iota(jnp.int32, (Y, Z), 0)
    wide_lane = lax.broadcasted_iota(jnp.int32, (Y, Z), 1)
    for x in range(X):
        for part, ref in ((0, v), (1, g)):
            half = 0.5 * ref[1, x]
            yu[x, part] = jnp.where(wide_row == Y - 1, 0.0, half + pltpu.roll(half, Y - 1, 0))
            yu[x, 2 + part] = jnp.where(wide_row == 0, 0.0, half + pltpu.roll(half, 1, 0))
            half = 0.5 * ref[2, x]
            zu[x, part] = jnp.where(wide_lane == Z - 1, 0.0, half + pltpu.roll(half, Z - 1, 1))
            zu[x, 2 + part] = jnp.where(wide_lane == 0, 0.0, half + pltpu.roll(half, 1, 1))
    def side_faces(i, carry):
        x, chunk = lax.div(i, zc), lax.rem(i, zc)
        zs = lanes_of(chunk)
        w, s = nodes_of(x + 1, zs)
        high = outflow(w, s, yu[x, 0, :, zs], yu[x, 1, :, zs], jnp.maximum)
        for k in range(8):
            acc[x, k, :, zs] = high[k] - jnp.where(row == 0, 0.0, pltpu.roll(high[k], 1, 0))
        low = outflow(w, s, yu[x, 2, :, zs], yu[x, 3, :, zs], jnp.minimum)
        for k in range(8):
            acc[x, k, :, zs] += (
                jnp.where(row == Y - 1, 0.0, pltpu.roll(low[k], Y - 1, 0)) - low[k]
            )
        return carry

    lax.fori_loop(0, X * zc, side_faces, 0)

    def wall_chunk(x, chunk):
        zs = slice(chunk * LANES, (chunk + 1) * LANES)
        w, s = nodes_of(x + 1, zs)
        high = outflow(w, s, zu[x, 0, :, zs], zu[x, 1, :, zs], jnp.maximum)
        for k in range(8):
            zp[x, k, :, zs] = pltpu.roll(high[k], 1, 1)
        low = outflow(w, s, zu[x, 2, :, zs], zu[x, 3, :, zs], jnp.minimum)
        for k in range(8):
            zm[x, k, :, zs] = pltpu.roll(low[k], LANES - 1, 1)
            acc[x, k, :, zs] += high[k] - low[k]

    def wall_faces(x, carry):
        for chunk in range(zc):
            wall_chunk(x, chunk)
        return carry

    lax.fori_loop(0, X, wall_faces, 0)

    def face_x(face, zs, left, right):
        mean = between(left, right)
        upper = outflow(*nodes_of(face, zs), *mean, jnp.maximum)
        lower = outflow(*nodes_of(face + 1, zs), *mean, jnp.minimum)
        for k in range(8):
            fx[face, k, :, zs] = upper[k] + lower[k]

    def inner_x(i, carry):
        face, zs = lax.div(i, zc) + 1, lanes_of(lax.rem(i, zc))
        face_x(face, zs, drift_of(face - 1, zs), drift_of(face, zs))
        return carry

    def outer_x(i, carry):
        zs = lanes_of(i)
        ahead = between((hvx[0, 0, :, zs], hvx[0, 1, :, zs]), drift_of(0, zs))
        upper = outflow(*nodes_of(0, zs), *ahead, jnp.maximum)
        for k in range(8):
            acc[0, k, :, zs] -= upper[k]
        after = between(drift_of(X - 1, zs), (hvx[1, 0, :, zs], hvx[1, 1, :, zs]))
        lower = outflow(*nodes_of(X + 1, zs), *after, jnp.minimum)
        for k in range(8):
            acc[X - 1, k, :, zs] += lower[k]
        return carry

    if X > 1:
        lax.fori_loop(0, (X - 1) * zc, inner_x, 0)

    await_group(NODES_SIDES)
    for side in range(2):
        into = y_outflow(y_r, side, upwinds[side], y_mean(1 - side))
        for k in range(8):
            y_face[side, k] += into[k]
        into = z_outflow(z_r, side, upwinds[side], z_mean(1 - side))
        for k in range(8):
            z_face[side, k] += jnp.where((bottom, top)[side], 0.0, into[k])

    def combine(x, carry):
        p = jnp.where(x == 0, 0, jnp.where(x == X - 1, 1, x + 1))
        for k in range(8):
            floor, ceiling = y_face[0, k, pl.ds(p, 1), :], y_face[1, k, pl.ds(p, 1), :]
            first = pltpu.roll(z_face[0, k], lax.rem(LANES - p, LANES), 1)
            last = pltpu.roll(z_face[1, k], LANES - 1 - p, 1)
            rises = [zp[x, k, :, c * LANES : (c + 1) * LANES] for c in range(zc)]
            falls = [zm[x, k, :, c * LANES : (c + 1) * LANES] for c in range(zc)]
            for c in range(zc):
                zs = slice(c * LANES, (c + 1) * LANES)
                before = jnp.where(lane == 0, rises[c - 1] if c else first, rises[c])
                after = jnp.where(lane == LANES - 1, falls[c + 1] if c < zc - 1 else last, falls[c])
                change = acc[x, k, :, zs] + (after - before)
                change = change + (fx[x + 1, k, :, zs] - fx[x, k, :, zs])
                acc[x, k, :, zs] = change + jnp.where(
                    row == Y - 1, ceiling[:, zs], jnp.where(row == 0, -floor[:, zs], 0.0)
                )
        return carry

    lax.fori_loop(0, X, combine, 0)
    await_group(NODES_X)
    lax.fori_loop(0, zc, outer_x, 0)

    every = pltpu.make_async_copy(
        table.at[pl.ds(0, count - 1)], table.at[pl.ds(0, count - 1)], all_sem.at[1]
    )
    every.wait()
    await_values(nb_send.at[0], sent[0])
    pltpu.make_async_copy(
        table.at[pl.ds(0, count - 1)], table.at[pl.ds(0, count - 1)], all_sem.at[0]
    ).wait()


def finish(sizes, acc, m, table, out_hbm, tot_hbm, stage, tot, sem):
    X, Y, Z = m.shape[1:]
    count = sizes[0] * sizes[1] * sizes[2]
    largest = jnp.max(table[:, 0:1, :], axis=0)
    step = cfl_number / (jnp.broadcast_to(largest, (Y, LANES)) + speed_eps)
    copies = []
    for k in range(8):
        for x in range(X):
            for c in range(Z // LANES):
                zs = slice(c * LANES, (c + 1) * LANES)
                stage[k, x, :, zs] = m[k, x, :, zs] - step * acc[x, k, :, zs]
        copies.append(pltpu.make_async_copy(stage.at[k], out_hbm.at[k], sem.at[k]))
        copies[-1].start()

    rows = table[:, 1:2, :]
    grid = rows.reshape(sizes + (1, LANES))

    def turned(axis, step):
        size = sizes[axis]
        cut = (size - step) % size
        if cut == 0:
            return grid
        return jnp.concatenate(
            [lax.slice_in_dim(grid, cut, size, axis=axis), lax.slice_in_dim(grid, 0, cut, axis=axis)],
            axis=axis,
        )

    group = lax.broadcasted_iota(jnp.int32, (1, LANES), 1) // 8
    net = jnp.zeros((1, LANES), jnp.float32)
    for axis in range(3):
        rise = jnp.sum((grid - turned(axis, 1)).reshape(count, 1, LANES), axis=0)
        fall = jnp.sum((turned(axis, -1) - grid).reshape(count, 1, LANES), axis=0)
        net = net + jnp.where(
            group == 1 + 2 * axis, rise, jnp.where(group == 2 + 2 * axis, fall, 0.0)
        )
    net = jnp.broadcast_to(net, (SUBLANES, LANES))
    change = functools.reduce(jnp.add, [pltpu.roll(net, LANES - 8 * n, 1) for n in range(1, 7)])
    both = jnp.sum(rows, axis=0) - step[0:1] * change[0:1]
    tot[...] = (both / float(count * X * Y * Z))[:, 0:8].reshape(8)
    copies.append(pltpu.make_async_copy(tot, tot_hbm, sem.at[8]))
    copies[-1].start()
    for copy in copies:
        copy.wait()


def shards(sizes, moments, velocity, drift):
    _, X, Y, Z = moments.shape
    count = sizes[0] * sizes[1] * sizes[2]
    f32 = jnp.float32
    vm = lambda *shape: pltpu.VMEM(shape, f32)
    near = pl.BlockSpec(memory_space=pltpu.VMEM)
    far = pl.BlockSpec(memory_space=pl.ANY)
    parts = pl.pallas_call(
        functools.partial(kernel, sizes),
        name="transport",
        out_shape=(vm(X, 8, Y, Z), vm(*moments.shape), vm(count, 2, LANES)),
        in_specs=[far] * 3,
        out_specs=(near,) * 3,
        scratch_shapes=[
            vm(3, X, Y, Z), vm(3, X, Y, Z), vm(X + 2, 8, Y, Z),
            vm(X + 1, 8, Y, Z), vm(X, 8, Y, Z), vm(X, 8, Y, Z), vm(X, 4, Y, Z), vm(X, 4, Y, Z),
            vm(2, 2, Y, Z), vm(2, 2, X, Z), vm(2, 2, X, Z), vm(2, Y, LANES), vm(2, Y, LANES),
            vm(2, Z // LANES, 8 * X, LANES), vm(2, Z // LANES, 8 * X, LANES),
            vm(2, Y, LANES), vm(2, Y, LANES),
            vm(2, 8, X, Z), vm(2, 8, Y, LANES), vm(14 * X * Y * Z // LANES, LANES),
            pltpu.SemaphoreType.DMA((2,)), pltpu.SemaphoreType.DMA((1,)),
            pltpu.SemaphoreType.DMA((4,)), pltpu.SemaphoreType.DMA((2,)),
            pltpu.SemaphoreType.REGULAR,
        ],
        compiler_params=pltpu.CompilerParams(
            collective_id=0, has_side_effects=True,
        ),
    )(moments, velocity, drift)
    return pl.pallas_call(
        functools.partial(finish, sizes),
        name="finish",
        out_shape=(jax.ShapeDtypeStruct(moments.shape, f32), jax.ShapeDtypeStruct((8,), f32)),
        in_specs=[near] * 3,
        out_specs=(far, far),
        scratch_shapes=[vm(*moments.shape), vm(8), pltpu.SemaphoreType.DMA((9,))],
    )(*(pltpu.with_memory_space_constraint(part, pltpu.VMEM) for part in parts))


def solution(mesh):
    spec = P(None, "gx", "gy", "gz")
    sizes = tuple(mesh.shape[a] for a in AXES)
    return jax.shard_map(
        functools.partial(shards, sizes), mesh=mesh, in_specs=(spec,) * 3,
        out_specs=(spec, P()), check_vma=False,
    )
```

```python
import functools

import jax
import jax.numpy as jnp
from jax import lax
from jax.experimental import pallas as pl
from jax.experimental.pallas import tpu as pltpu
from jax.sharding import PartitionSpec as P

SWEEPS = 6
EARLY_NODES = 4
AXES = ("gx", "gy", "gz")
LANES = 128
SUBLANES = 8

cfl_number = 0.4
speed_eps = 1e-06
pair_list = ((0, 1), (0, 2), (0, 3), (1, 2), (1, 3), (2, 3))


def entry_key(i, j):
    return (min(i, j), max(i, j))


def scaled(scale, value):
    return value if scale is None else scale * value


def sheared(alpha, beta, near, far):
    if near is None and far is None:
        return None, None
    if near is None:
        return -(alpha * far), far
    if far is None:
        return near, beta * near
    return near - alpha * far, far + beta * near


def recurrence(moment):
    levels = list(moment)
    before = None
    inverse = 1.0 / levels[0]
    ratios = [levels[1] * inverse]
    alphas = [ratios[0]]
    betas = [levels[0]]
    for level in range(1, 4):
        fresh = [None] * 8
        for column in range(level, 8 - level):
            value = levels[column + 1] - alphas[level - 1] * levels[column]
            if level > 1:
                value = value - betas[level - 1] * before[column]
            fresh[column] = value
        betas.append(fresh[level] * inverse)
        inverse = 1.0 / fresh[level]
        ratios.append(fresh[level + 1] * inverse)
        alphas.append(ratios[level] - ratios[level - 1])
        before, levels = levels, fresh
    return alphas, betas


def begin(moment):
    diag, betas = recurrence(moment)
    table = {(i, j): None for i in range(4) for j in range(i + 1, 4)}
    for i in range(3):
        table[i, i + 1] = 2.0
    scale = [None, betas[1]]
    for i in range(2, 4):
        scale.append(betas[i] / scale[i - 1])
    return diag, table, scale, [1.0, None, None, None]


def sweep(state, sweeps):
    diag, table, scale, first = state
    for _ in range(sweeps):
        for p, q in pair_list:
            entry = table[p, q]
            if entry is None:
                continue
            spread = diag[q] - diag[p]
            left = scaled(scale[p], entry)
            right = scaled(scale[q], entry)
            square = spread * spread + left * right
            r = lax.rsqrt(square)
            r = jnp.where(spread >= 0, r, -r)
            both = spread + square * r
            turn = 1.0 / both
            half = 0.5 * both
            alpha = right * turn
            beta = left * turn
            shrink = half * r
            scale[p] = scaled(scale[p], shrink)
            scale[q] = scaled(scale[q], shrink)
            for rest in range(4):
                if rest not in (p, q):
                    a, b = entry_key(rest, p), entry_key(rest, q)
                    table[a], table[b] = sheared(alpha, beta, table[a], table[b])
            diag[p], diag[q] = diag[q] - half, diag[p] + half
            table[p, q] = None
            first[p], first[q] = sheared(alpha, beta, first[p], first[q])


def quadrature(number, state):
    diag, table, scale, first = state
    return [number * (scale[i] * (first[i] * first[i])) for i in range(4)], diag


def outflow(weights, sizes, mean_speed, mean_drift, upwind):
    sums = None
    for w, s in zip(weights, sizes):
        term = w * upwind(mean_speed + mean_drift * s, 0.0)
        terms = [term]
        for _ in range(7):
            term = term * s
            terms.append(term)
        sums = terms if sums is None else [a + b for a, b in zip(sums, terms)]
    return sums


def kernel(
    sizes, m_hbm, v_hbm, g_hbm, acc, m, table,
    vg, nodes, fx, zp, zm, yu, zu,
    hvx, vy_s, vy_r, vz_s, vz_r, y_s, y_r, z_s, z_r, y_face, z_face, tally,
    in_sem, nb_send, nb_recv, all_sem, plane_sem,
):
    X, Y, Z = m.shape[1:]
    count = sizes[0] * sizes[1] * sizes[2]
    v, g = vg.at[:, 0], vg.at[:, 1]
    zc = Z // LANES
    at = [lax.axis_index(a) for a in AXES]
    me = (at[0] * sizes[1] + at[1]) * sizes[2] + at[2]
    row = lax.broadcasted_iota(jnp.int32, (Y, LANES), 0)
    lane = lax.broadcasted_iota(jnp.int32, (Y, LANES), 1)
    bottom = at[2] == 0
    top = at[2] == sizes[2] - 1

    def along(axis, step):
        return lax.rem(at[axis] + step + sizes[axis], sizes[axis])

    def beside(axis, step):
        place = list(at)
        place[axis] = along(axis, step)
        return tuple(place)

    edge = [0] if X == 1 else [0, X - 1]
    inner = list(range(1, X - 1))

    def await_values(sem, number):
        rows = tally.at[pl.ds(0, number // LANES)]
        pltpu.make_async_copy(rows, rows, sem).wait()

    def load(layers, sem):
        for x in layers:
            for k in range(8):
                pltpu.make_async_copy(m_hbm.at[k, x], m.at[k, x], sem).start()
        return 8 * len(layers) * Y * Z

    first_load = load(edge, in_sem.at[0])
    for far, ref in ((v_hbm, v), (g_hbm, g)):
        for d in range(3):
            pltpu.make_async_copy(far.at[d], ref.at[d], in_sem.at[1]).start()
    second_load = load(inner, in_sem.at[1]) + 6 * X * Y * Z

    barrier = pltpu.get_barrier_semaphore()
    xs = [along(0, i) for i in range(sizes[0])]
    zs_ = [along(2, i) for i in range(sizes[2])]
    plane = [
        (xs[i], at[1], zs_[j]) for i in range(sizes[0]) for j in range(sizes[2]) if i or j
    ]
    line = [(at[0], along(1, i), at[2]) for i in range(1, sizes[1])]
    for place in plane + line:
        pl.semaphore_signal(
            barrier, inc=1, device_id=place, device_id_type=pl.DeviceIdType.MESH
        )

    V_SIDES, V_X, NODES_X, NODES_SIDES = range(4)
    sent, due = [0], [0] * 4

    def send(src, dst, axis, step, group, counted=True):
        pltpu.make_async_remote_copy(
            src_ref=src, dst_ref=dst, send_sem=nb_send.at[0], recv_sem=nb_recv.at[group],
            device_id=beside(axis, step), device_id_type=pl.DeviceIdType.MESH,
        ).start()
        number = functools.reduce(lambda p, q: p * q, src.shape, 1) if counted else 0
        sent[0] += number
        due[group] += number

    def await_group(group):
        await_values(nb_recv.at[group], due[group])

    order = edge + inner
    columns = [jnp.zeros((Y, LANES), jnp.float32)] * 2

    def moments_of(layers, k):
        return jnp.concatenate([m[k, x] for x in layers], axis=0)

    def start(layers):
        return begin([moments_of(layers, k) for k in range(8)])

    def solve(layers, state):
        sweep(state, SWEEPS)
        weights, places = quadrature(moments_of(layers, 0), state)
        for n, x in enumerate(layers):
            for i in range(4):
                nodes[x + 1, i] = weights[i][n * Y : (n + 1) * Y]
                nodes[x + 1, 4 + i] = places[i][n * Y : (n + 1) * Y]
            for i, value in enumerate(weights + places):
                value = value[n * Y : (n + 1) * Y]
                p = order.index(x)
                for c in range(zc):
                    part = value[:, c * LANES : (c + 1) * LANES]
                    y_s[0, c, 8 * p + i : 8 * p + i + 1, :] = part[Y - 1 : Y]
                    y_s[1, c, 8 * p + i : 8 * p + i + 1, :] = part[0:1]
                spot = i * X + p
                for side, edge_lane in ((0, LANES - 1), (1, 0)):
                    tile = value[:, Z - LANES : Z] if side == 0 else value[:, 0:LANES]
                    turn = (spot - edge_lane) % LANES
                    tile = pltpu.roll(tile, turn, 1) if turn else tile
                    columns[side] = jnp.where(lane == spot, tile, columns[side])

    def fastest(x):
        speed = None
        for d in range(3):
            vd, gd = v[d, x], g[d, x]
            parts = [jnp.abs(vd + gd * nodes[x + 1, 4 + i]) for i in range(4)]
            largest = jnp.maximum(
                jnp.maximum(parts[0], parts[1]), jnp.maximum(parts[2], parts[3])
            )
            speed = largest if speed is None else speed + largest
        return speed

    await_values(in_sem.at[0], first_load)
    solve(edge, start(edge))
    await_values(in_sem.at[1], second_load)
    packs = [jnp.zeros((Y, LANES), jnp.float32)] * 2
    for p, x in enumerate(order):
        for part, ref in ((0, v), (1, g)):
            vy_s[0, part, p : p + 1, :] = ref[1, x, Y - 1 : Y, :]
            vy_s[1, part, p : p + 1, :] = ref[1, x, 0:1, :]
            spot = part * X + p
            tile = pltpu.roll(ref[2, x, :, Z - LANES : Z], spot + 1, 1)
            packs[0] = jnp.where(lane == spot, tile, packs[0])
            tile = ref[2, x, :, 0:LANES]
            tile = pltpu.roll(tile, spot, 1) if spot else tile
            packs[1] = jnp.where(lane == spot, tile, packs[1])
    for side in range(2):
        vz_s[side] = packs[side]
    pl.semaphore_wait(barrier, len(plane) + len(line))
    for side, step in ((0, 1), (1, -1)):
        send(vy_s.at[side], vy_r.at[side], 1, step, V_SIDES)
        send(vz_s.at[side], vz_r.at[side], 2, step, V_SIDES)
    for side, step, x in ((0, 1, X - 1), (1, -1, 0)):
        send(vg.at[0, :, x], hvx.at[side], 0, step, V_X)

    def send_x(part, counted=True):
        send(nodes.at[1, part], nodes.at[X + 1, part], 0, -1, NODES_X, counted)
        send(nodes.at[X, part], nodes.at[0, part], 0, 1, NODES_X, counted)

    def send_y(start, size):
        rows = pl.ds(8 * start, 8 * size)
        send(y_s.at[0, :, rows], y_r.at[0, :, rows], 1, 1, NODES_SIDES)
        send(y_s.at[1, :, rows], y_r.at[1, :, rows], 1, -1, NODES_SIDES)

    for place in line:
        pl.semaphore_signal(
            plane_sem, inc=1, device_id=place, device_id_type=pl.DeviceIdType.MESH
        )

    def fold(value):
        value = functools.reduce(
            jnp.add, [value[i : i + SUBLANES, :] for i in range(0, value.shape[0], SUBLANES)]
        )
        return functools.reduce(
            jnp.add, [value[:, i : i + LANES] for i in range(0, value.shape[1], LANES)]
        )

    send_y(0, len(edge))
    send_x(pl.ds(0, EARLY_NODES))

    if inner:
        solve(inner, start(inner))
        send_y(len(edge), len(inner))
    for side in range(2):
        z_s[side] = columns[side]
    for side, step in ((0, 1), (1, -1)):
        send(z_s.at[side], z_r.at[side], 2, step, NODES_SIDES)
    m_sums = [functools.reduce(jnp.add, [fold(m[k, x]) for x in range(X)]) for k in range(8)]
    best = functools.reduce(jnp.maximum, [fastest(x) for x in range(X)])

    def lanes_of(chunk):
        return pl.ds(pl.multiple_of(chunk * LANES, LANES), LANES)

    def nodes_of(layer, zs, ys=slice(None)):
        return (
            [nodes[layer, i, ys, zs] for i in range(4)],
            [nodes[layer, 4 + i, ys, zs] for i in range(4)],
        )

    def drift_of(x, zs):
        return v[0, x, :, zs], g[0, x, :, zs]

    def between(left, right):
        return 0.5 * (left[0] + right[0]), 0.5 * (left[1] + right[1])

    def inside():
        wide_row = lax.broadcasted_iota(jnp.int32, (Y, Z), 0)
        wide_lane = lax.broadcasted_iota(jnp.int32, (Y, Z), 1)
        for x in range(X):
            for part, ref in ((0, v), (1, g)):
                half = 0.5 * ref[1, x]
                yu[x, part] = jnp.where(wide_row == Y - 1, 0.0, half + pltpu.roll(half, Y - 1, 0))
                yu[x, 2 + part] = jnp.where(wide_row == 0, 0.0, half + pltpu.roll(half, 1, 0))
                half = 0.5 * ref[2, x]
                zu[x, part] = jnp.where(wide_lane == Z - 1, 0.0, half + pltpu.roll(half, Z - 1, 1))
                zu[x, 2 + part] = jnp.where(wide_lane == 0, 0.0, half + pltpu.roll(half, 1, 1))
        def side_faces(i, carry):
            x, chunk = lax.div(i, zc), lax.rem(i, zc)
            zs = lanes_of(chunk)
            w, s = nodes_of(x + 1, zs)
            high = outflow(w, s, yu[x, 0, :, zs], yu[x, 1, :, zs], jnp.maximum)
            for k in range(8):
                acc[x, k, :, zs] = high[k] - jnp.where(row == 0, 0.0, pltpu.roll(high[k], 1, 0))
            low = outflow(w, s, yu[x, 2, :, zs], yu[x, 3, :, zs], jnp.minimum)
            for k in range(8):
                acc[x, k, :, zs] += (
                    jnp.where(row == Y - 1, 0.0, pltpu.roll(low[k], Y - 1, 0)) - low[k]
                )
            return carry

        lax.fori_loop(0, X * zc, side_faces, 0)

        def wall_chunk(x, chunk):
            zs = slice(chunk * LANES, (chunk + 1) * LANES)
            w, s = nodes_of(x + 1, zs)
            high = outflow(w, s, zu[x, 0, :, zs], zu[x, 1, :, zs], jnp.maximum)
            for k in range(8):
                zp[x, k, :, zs] = pltpu.roll(high[k], 1, 1)
            low = outflow(w, s, zu[x, 2, :, zs], zu[x, 3, :, zs], jnp.minimum)
            for k in range(8):
                zm[x, k, :, zs] = pltpu.roll(low[k], LANES - 1, 1)
                acc[x, k, :, zs] += high[k] - low[k]

        def wall_faces(x, carry):
            for chunk in range(zc):
                wall_chunk(x, chunk)
            return carry

        lax.fori_loop(0, X, wall_faces, 0)

    last_nodes = pl.ds(EARLY_NODES, 8 - EARLY_NODES)
    @pl.when(at[1] == 0)
    def _():
        send_x(last_nodes)
        inside()

    await_group(V_SIDES)
    await_group(V_X)

    upwinds = (jnp.maximum, jnp.minimum)

    def y_mean(side):
        return [0.5 * (vy_s[side, part] + vy_r[1 - side, part]) for part in range(2)]

    def y_outflow(source, side, upwind, mean):
        rows = [
            jnp.concatenate([source[side, c, pl.ds(i, X, stride=8), :] for c in range(zc)], axis=1)
            for i in range(8)
        ]
        return outflow(rows[:4], rows[4:], *mean, upwind)

    def z_mean(side):
        mean = 0.5 * (vz_s[side] + vz_r[1 - side])
        return [mean, pltpu.roll(mean, LANES - X, 1)]

    def z_outflow(source, side, upwind, mean):
        tile = source[side]
        parts = [tile] + [pltpu.roll(tile, LANES - i * X, 1) for i in range(1, 8)]
        return outflow(parts[:4], parts[4:], *mean, upwind)

    y_sums = [y_outflow(y_s, side, upwinds[side], y_mean(side)) for side in range(2)]
    z_sums = [
        [
            jnp.where((lane < X) & jnp.logical_not((top, bottom)[side]), value, 0.0)
            for value in z_outflow(z_s, side, upwinds[side], z_mean(side))
        ]
        for side in range(2)
    ]

    for side in range(2):
        for k in range(8):
            y_face[1 - side, k] = y_sums[side][k]
            z_face[1 - side, k] = z_sums[side][k]


    def side_x(i, sums):
        zs = slice(i * LANES, (i + 1) * LANES)
        ahead = between((hvx[0, 0, :, zs], hvx[0, 1, :, zs]), drift_of(0, zs))
        after = between(drift_of(X - 1, zs), (hvx[1, 0, :, zs], hvx[1, 1, :, zs]))
        upper = outflow(*nodes_of(X, zs), *after, jnp.maximum)
        lower = outflow(*nodes_of(1, zs), *ahead, jnp.minimum)
        for k in range(8):
            fx[X, k, :, zs] = upper[k]
            fx[0, k, :, zs] = lower[k]
        return tuple(a + fold(b) for a, b in zip(sums, upper + lower))

    zero = jnp.zeros((SUBLANES, LANES), jnp.float32)
    x_sums = (zero,) * 16
    for i in range(zc):
        x_sums = side_x(i, x_sums)

    tile_row = lax.broadcasted_iota(jnp.int32, (SUBLANES, LANES), 0)
    tile_lane = lax.broadcasted_iota(jnp.int32, (SUBLANES, LANES), 1)

    def narrow(value):
        return functools.reduce(
            jnp.add, [value[:, i : i + LANES] for i in range(0, value.shape[1], LANES)]
        )

    packed = zero
    groups = [m_sums, x_sums[:8], x_sums[8:]] + [[narrow(a) for a in y] for y in y_sums] + z_sums
    for n, sums in enumerate(groups):
        block = zero
        for k in range(8):
            block = jnp.where(tile_row == k, jnp.sum(sums[k], axis=0, keepdims=True), block)
        value = jnp.sum(block, axis=1, keepdims=True)
        packed = jnp.where(tile_lane == tile_row + 8 * n, value, packed)
    packed = jnp.sum(packed, axis=0, keepdims=True)
    best = functools.reduce(
        jnp.maximum,
        [best[i : i + SUBLANES, j : j + LANES]
         for i in range(0, Y, SUBLANES) for j in range(0, Z, LANES)],
    )
    best = jnp.max(jnp.max(best, axis=0, keepdims=True), axis=1, keepdims=True)
    table[me, 0:1] = jnp.broadcast_to(best, (1, LANES))
    table[me, 1:2] = packed

    pl.semaphore_wait(plane_sem, len(line))

    def spread(j, carry):
        place = jnp.where(j >= me, j + 1, j)
        pltpu.make_async_remote_copy(
            src_ref=table.at[me], dst_ref=table.at[me],
            send_sem=all_sem.at[0], recv_sem=all_sem.at[1],
            device_id=place, device_id_type=pl.DeviceIdType.LOGICAL,
        ).start()
        return carry

    lax.fori_loop(0, count - 1, spread, 0)
    @pl.when(at[1] != 0)
    def _():
        send_x(last_nodes, False)
        inside()


    def face_x(face, zs, left, right):
        mean = between(left, right)
        upper = outflow(*nodes_of(face, zs), *mean, jnp.maximum)
        lower = outflow(*nodes_of(face + 1, zs), *mean, jnp.minimum)
        for k in range(8):
            fx[face, k, :, zs] = upper[k] + lower[k]

    def inner_x(i, carry):
        face, zs = lax.div(i, zc) + 1, lanes_of(lax.rem(i, zc))
        face_x(face, zs, drift_of(face - 1, zs), drift_of(face, zs))
        return carry

    if X > 1:
        lax.fori_loop(0, (X - 1) * zc, inner_x, 0)

    def outer_x(i, carry):
        zs = lanes_of(i)
        ahead = between((hvx[0, 0, :, zs], hvx[0, 1, :, zs]), drift_of(0, zs))
        upper = outflow(*nodes_of(0, zs), *ahead, jnp.maximum)
        for k in range(8):
            acc[0, k, :, zs] -= upper[k]
        after = between(drift_of(X - 1, zs), (hvx[1, 0, :, zs], hvx[1, 1, :, zs]))
        lower = outflow(*nodes_of(X + 1, zs), *after, jnp.minimum)
        for k in range(8):
            acc[X - 1, k, :, zs] += lower[k]
        return carry

    await_group(NODES_SIDES)
    for side in range(2):
        into = y_outflow(y_r, side, upwinds[side], y_mean(1 - side))
        for k in range(8):
            y_face[side, k] += into[k]
        into = z_outflow(z_r, side, upwinds[side], z_mean(1 - side))
        for k in range(8):
            z_face[side, k] += jnp.where((bottom, top)[side], 0.0, into[k])

    def combine(x, carry):
        p = jnp.where(x == 0, 0, jnp.where(x == X - 1, 1, x + 1))
        for k in range(8):
            floor, ceiling = y_face[0, k, pl.ds(p, 1), :], y_face[1, k, pl.ds(p, 1), :]
            first = pltpu.roll(z_face[0, k], lax.rem(LANES - p, LANES), 1)
            last = pltpu.roll(z_face[1, k], LANES - 1 - p, 1)
            rises = [zp[x, k, :, c * LANES : (c + 1) * LANES] for c in range(zc)]
            falls = [zm[x, k, :, c * LANES : (c + 1) * LANES] for c in range(zc)]
            for c in range(zc):
                zs = slice(c * LANES, (c + 1) * LANES)
                before = jnp.where(lane == 0, rises[c - 1] if c else first, rises[c])
                after = jnp.where(lane == LANES - 1, falls[c + 1] if c < zc - 1 else last, falls[c])
                change = acc[x, k, :, zs] + (after - before)
                change = change + (fx[x + 1, k, :, zs] - fx[x, k, :, zs])
                acc[x, k, :, zs] = change + jnp.where(
                    row == Y - 1, ceiling[:, zs], jnp.where(row == 0, -floor[:, zs], 0.0)
                )
        return carry

    lax.fori_loop(0, X, combine, 0)
    await_group(NODES_X)
    lax.fori_loop(0, zc, outer_x, 0)

    every = pltpu.make_async_copy(
        table.at[pl.ds(0, count - 1)], table.at[pl.ds(0, count - 1)], all_sem.at[1]
    )
    every.wait()
    await_values(nb_send.at[0], sent[0])
    pltpu.make_async_copy(
        table.at[pl.ds(0, count - 1)], table.at[pl.ds(0, count - 1)], all_sem.at[0]
    ).wait()


def finish(sizes, acc, m, table, out_hbm, tot_hbm, stage, tot, sem):
    X, Y, Z = m.shape[1:]
    count = sizes[0] * sizes[1] * sizes[2]
    largest = jnp.max(table[:, 0:1, :], axis=0)
    step = cfl_number / (jnp.broadcast_to(largest, (Y, LANES)) + speed_eps)
    copies = []
    for k in range(8):
        for x in range(X):
            for c in range(Z // LANES):
                zs = slice(c * LANES, (c + 1) * LANES)
                stage[k, x, :, zs] = m[k, x, :, zs] - step * acc[x, k, :, zs]
            if x % 2:
                part = pl.ds(x - 1, 2)
                copies.append(pltpu.make_async_copy(stage.at[k, part], out_hbm.at[k, part], sem.at[2 * k + x // 2]))
                copies[-1].start()

    rows = table[:, 1:2, :]
    grid = rows.reshape(sizes + (1, LANES))

    def turned(axis, step):
        size = sizes[axis]
        cut = (size - step) % size
        if cut == 0:
            return grid
        return jnp.concatenate(
            [lax.slice_in_dim(grid, cut, size, axis=axis), lax.slice_in_dim(grid, 0, cut, axis=axis)],
            axis=axis,
        )

    group = lax.broadcasted_iota(jnp.int32, (1, LANES), 1) // 8
    net = jnp.zeros((1, LANES), jnp.float32)
    for axis in range(3):
        rise = jnp.sum((grid - turned(axis, 1)).reshape(count, 1, LANES), axis=0)
        fall = jnp.sum((turned(axis, -1) - grid).reshape(count, 1, LANES), axis=0)
        net = net + jnp.where(
            group == 1 + 2 * axis, rise, jnp.where(group == 2 + 2 * axis, fall, 0.0)
        )
    net = jnp.broadcast_to(net, (SUBLANES, LANES))
    change = functools.reduce(jnp.add, [pltpu.roll(net, LANES - 8 * n, 1) for n in range(1, 7)])
    both = jnp.sum(rows, axis=0) - step[0:1] * change[0:1]
    tot[...] = (both / float(count * X * Y * Z))[:, 0:8].reshape(8)
    copies.append(pltpu.make_async_copy(tot, tot_hbm, sem.at[16]))
    copies[-1].start()
    for copy in copies:
        copy.wait()


def shards(sizes, moments, velocity, drift):
    _, X, Y, Z = moments.shape
    count = sizes[0] * sizes[1] * sizes[2]
    f32 = jnp.float32
    vm = lambda *shape: pltpu.VMEM(shape, f32)
    near = pl.BlockSpec(memory_space=pltpu.VMEM)
    far = pl.BlockSpec(memory_space=pl.ANY)
    parts = pl.pallas_call(
        functools.partial(kernel, sizes),
        name="transport",
        out_shape=(vm(X, 8, Y, Z), vm(*moments.shape), vm(count, 2, LANES)),
        in_specs=[far] * 3,
        out_specs=(near,) * 3,
        scratch_shapes=[
            vm(3, 2, X, Y, Z), vm(X + 2, 8, Y, Z),
            vm(X + 1, 8, Y, Z), vm(X, 8, Y, Z), vm(X, 8, Y, Z), vm(X, 4, Y, Z), vm(X, 4, Y, Z),
            vm(2, 2, Y, Z), vm(2, 2, X, Z), vm(2, 2, X, Z), vm(2, Y, LANES), vm(2, Y, LANES),
            vm(2, Z // LANES, 8 * X, LANES), vm(2, Z // LANES, 8 * X, LANES),
            vm(2, Y, LANES), vm(2, Y, LANES),
            vm(2, 8, X, Z), vm(2, 8, Y, LANES), vm(14 * X * Y * Z // LANES, LANES),
            pltpu.SemaphoreType.DMA((2,)), pltpu.SemaphoreType.DMA((1,)),
            pltpu.SemaphoreType.DMA((4,)), pltpu.SemaphoreType.DMA((2,)),
            pltpu.SemaphoreType.REGULAR,
        ],
        compiler_params=pltpu.CompilerParams(
            collective_id=0, has_side_effects=True,
        ),
    )(moments, velocity, drift)
    return pl.pallas_call(
        functools.partial(finish, sizes),
        name="finish",
        out_shape=(jax.ShapeDtypeStruct(moments.shape, f32), jax.ShapeDtypeStruct((8,), f32)),
        in_specs=[near] * 3,
        out_specs=(far, far),
        scratch_shapes=[vm(*moments.shape), vm(8), pltpu.SemaphoreType.DMA((17,))],
    )(*(pltpu.with_memory_space_constraint(part, pltpu.VMEM) for part in parts))


def solution(mesh):
    spec = P(None, "gx", "gy", "gz")
    sizes = tuple(mesh.shape[a] for a in AXES)
    return jax.shard_map(
        functools.partial(shards, sizes), mesh=mesh, in_specs=(spec,) * 3,
        out_specs=(spec, P()), check_vma=False,
    )
```
